8 devices in a mesh: dp: 1 (over z), tp: 2 (over y), cp: 4 (over x, core).
Axes of the slice: x: 2, y: 2, z: 1, core: 2. Of those that a mesh axis runs over, the one named last changes fastest.
Arguments:
- hidden: bfloat16 [2048, 8192], P(('dp', 'cp'))
- tok_pos: int32 [2048], P(('dp', 'cp'))
- norm_gain: float32 [8192], replicated
- w_query: bfloat16 [8192, 8192], P(None, 'tp')
- w_key: bfloat16 [8192, 1024], P(None, 'tp')
- w_value: bfloat16 [8192, 1024], P(None, 'tp')
- w_out: bfloat16 [8192, 8192], P('tp')
Outputs:
- output 1: bfloat16 [2048, 8192], P(('dp', 'cp'))
- output 2: bfloat16 [2048, 8, 128], P(('dp', 'cp'), 'tp')
- output 3: bfloat16 [2048, 8, 128], P(('dp', 'cp'), 'tp')
All inputs are finite; a program needn't handle non-finite values.
Results may differ from the reference program's by a relative error of at most 0.00490281.
Values are sent between devices in bfloat16 or wider.
A program may use at most 1 GiB of HBM per device.

```python
import math
import jax
import jax.numpy as jnp
from jax import lax

D = 8192
HEADS = 64
KV_HEADS = 8
HEAD = 128
SEQ = 2048
RUN_LEN = 128
Q_BLOCK = 128
THETA = 1000000
EPS = 1e-5


def setup_inputs(seed: int = 0, part: int = 0) -> dict:
    shared = jax.random.split(jax.random.key(seed), 5)
    local = jax.random.split(jax.random.fold_in(jax.random.key(seed + 1), part), 4)
    run_order = jax.random.permutation(local[0], SEQ // RUN_LEN)
    tok_pos = (run_order[:, None] * RUN_LEN + jnp.arange(RUN_LEN)[None, :]).reshape(SEQ).astype(jnp.int32)
    waves = jax.random.normal(local[1], (4, D), jnp.float32)
    phases = jax.random.uniform(local[2], (4,), jnp.float32, 0.0, 2.0 * math.pi)
    cycles = jnp.array([0.5, 1.0, 1.5, 2.5], jnp.float32)
    angle = tok_pos.astype(jnp.float32)[:, None] * (cycles * (2.0 * math.pi / SEQ))[None, :] + phases[None, :]
    signal = jnp.dot(jnp.cos(angle), waves)
    noise = jax.random.normal(local[3], (SEQ, D), jnp.float32)
    hidden = (0.25 * signal + 0.2 * noise).astype(jnp.bfloat16)
    norm_gain = 1.0 + 0.3 * jax.random.normal(shared[0], (D,), jnp.float32)
    w_query = (jax.random.normal(shared[1], (D, HEADS * HEAD), jnp.float32) * D ** -0.5).astype(jnp.bfloat16)
    w_key = (jax.random.normal(shared[2], (D, KV_HEADS * HEAD), jnp.float32) * D ** -0.5).astype(jnp.bfloat16)
    w_value = (jax.random.normal(shared[3], (D, KV_HEADS * HEAD), jnp.float32) * D ** -0.5).astype(jnp.bfloat16)
    w_out = (jax.random.normal(shared[4], (HEADS * HEAD, D), jnp.float32) * (HEADS * HEAD) ** -0.5).astype(jnp.bfloat16)
    return {"hidden": hidden, "tok_pos": tok_pos, "norm_gain": norm_gain, "w_query": w_query, "w_key": w_key, "w_value": w_value, "w_out": w_out}


def rope_tables(tok_pos):
    inv_freq = 1.0 / (THETA ** (jnp.arange(0, HEAD, 2, dtype=jnp.float32) / HEAD))
    angles = tok_pos.astype(jnp.float32)[:, None] * inv_freq[None, :]
    return jnp.cos(angles)[:, None, :], jnp.sin(angles)[:, None, :]


def rotate_half(head_vecs, cos_tab, sin_tab):
    half_dim = head_vecs.shape[-1] // 2
    first_half = head_vecs[..., :half_dim].astype(jnp.float32)
    second_half = head_vecs[..., half_dim:].astype(jnp.float32)
    rotated = jnp.concatenate([first_half * cos_tab - second_half * sin_tab, second_half * cos_tab + first_half * sin_tab], axis=-1)
    return rotated.astype(jnp.bfloat16)


def reference(hidden, tok_pos, norm_gain, w_query, w_key, w_value, w_out):
    q_per_kv = HEADS // KV_HEADS
    n_blocks = SEQ // Q_BLOCK
    hid_f32 = hidden.astype(jnp.float32)
    normed = (hid_f32 * lax.rsqrt(jnp.mean(hid_f32 * hid_f32, axis=-1, keepdims=True) + EPS) * norm_gain).astype(jnp.bfloat16)
    queries = jnp.dot(normed, w_query, preferred_element_type=jnp.float32).astype(jnp.bfloat16).reshape(SEQ, HEADS, HEAD)
    keys_raw = jnp.dot(normed, w_key, preferred_element_type=jnp.float32).astype(jnp.bfloat16).reshape(SEQ, KV_HEADS, HEAD)
    values = jnp.dot(normed, w_value, preferred_element_type=jnp.float32).astype(jnp.bfloat16).reshape(SEQ, KV_HEADS, HEAD)
    cos_tab, sin_tab = rope_tables(tok_pos)
    q_rot = rotate_half(queries, cos_tab, sin_tab)
    k_rot = rotate_half(keys_raw, cos_tab, sin_tab)
    attn_scale = HEAD ** -0.5
    k_heads = jnp.transpose(k_rot, (1, 0, 2)).astype(jnp.float32)
    v_heads = jnp.transpose(values, (1, 0, 2)).astype(jnp.float32)
    q_blocks = jnp.transpose(q_rot.reshape(n_blocks, Q_BLOCK, KV_HEADS, q_per_kv, HEAD), (0, 2, 1, 3, 4))
    pos_blocks = tok_pos.reshape(n_blocks, Q_BLOCK)

    def one_block(block_in):
        q_blk, pos_blk = block_in
        allowed = tok_pos[None, :] <= pos_blk[:, None]

        def one_head(head_in):
            q_head, k_head, v_head = head_in
            scores = jnp.einsum("qgd,td->gqt", q_head.astype(jnp.float32), k_head) * attn_scale
            scores = jnp.where(allowed[None], scores, -jnp.inf)
            softmaxed = jax.nn.softmax(scores, axis=-1)
            return jnp.einsum("gqt,td->qgd", softmaxed, v_head)

        return lax.map(one_head, (q_blk, k_heads, v_heads))

    context = lax.map(one_block, (q_blocks, pos_blocks))
    attn_out = jnp.transpose(context, (0, 2, 1, 3, 4)).reshape(SEQ, HEADS * HEAD).astype(jnp.bfloat16)
    attn_proj = jnp.dot(attn_out, w_out, preferred_element_type=jnp.float32)
    return (hid_f32 + attn_proj).astype(jnp.bfloat16), k_rot, values
```

```python
import functools

import jax
import jax.numpy as jnp
from jax import lax
from jax.experimental import pallas as pl
from jax.experimental.pallas import tpu as pltpu
from jax.sharding import PartitionSpec as P

HEAD = 128
THETA = 1000000
EPS = 1e-5
NEG_BIG = -1e30
Q_ROWS = 128
K_ROWS = 256
COLS = 1024
ANY = pl.BlockSpec(memory_space=pl.ANY)


def rms_normed(hid_f32, norm_gain):
    scaled = hid_f32 * lax.rsqrt(jnp.mean(hid_f32 * hid_f32, axis=-1, keepdims=True) + EPS)
    return (scaled * norm_gain).astype(jnp.bfloat16)


def rope_tables(tok_pos):
    inv_freq = 1.0 / (THETA ** (jnp.arange(0, HEAD, 2, dtype=jnp.float32) / HEAD))
    angles = tok_pos.astype(jnp.float32)[:, None] * inv_freq[None, :]
    cos, sin = jnp.cos(angles), jnp.sin(angles)
    return jnp.concatenate([cos, cos], axis=-1), jnp.concatenate([-sin, sin], axis=-1)


def rope_kernel(heads, x_ref, cos_ref, sin_ref, o_ref):
    for h in range(heads):
        cols = slice(h * HEAD, (h + 1) * HEAD)
        x = x_ref[:, cols].astype(jnp.float32)
        o_ref[:, cols] = (x * cos_ref[...] + pltpu.roll(x, HEAD // 2, 1) * sin_ref[...]).astype(jnp.bfloat16)


def rope(x, cos, sin):
    rows, cols = x.shape
    return pl.pallas_call(
        functools.partial(rope_kernel, cols // HEAD),
        out_shape=jax.ShapeDtypeStruct((rows, cols), jnp.bfloat16),
        cost_estimate=pl.CostEstimate(flops=rows * cols * 4, bytes_accessed=rows * cols * 4, transcendentals=0),
    )(x, cos, sin)


def attn_kernel(blocks, q_per_kv, kmin_ref, qmax_ref, q_ref, cos_ref, sin_ref, qpos_ref, kpos_ref, *rest):
    k_refs, v_refs = rest[:blocks], rest[blocks:2 * blocks]
    o_ref, q_s, m_s, l_s, acc_s = rest[2 * blocks:]
    qi = pl.program_id(1)
    scale = HEAD ** -0.5
    for g in range(q_per_kv):
        x = q_ref[:, g * HEAD:(g + 1) * HEAD].astype(jnp.float32)
        q_s[g] = (x * cos_ref[...] + pltpu.roll(x, HEAD // 2, 1) * sin_ref[...]).astype(jnp.bfloat16)
    m_s[...] = jnp.full_like(m_s, NEG_BIG)
    l_s[...] = jnp.zeros_like(l_s)
    acc_s[...] = jnp.zeros_like(acc_s)
    per = k_refs[0].shape[0] // K_ROWS
    for b in range(blocks):
        for c in range(per):
            idx = b * per + c

            @pl.when(kmin_ref[idx] <= qmax_ref[qi])
            def _(b=b, c=c, idx=idx):
                k = k_refs[b][c * K_ROWS:(c + 1) * K_ROWS, :]
                v = v_refs[b][c * K_ROWS:(c + 1) * K_ROWS, :]
                allowed = kpos_ref[:, idx * K_ROWS:(idx + 1) * K_ROWS] <= qpos_ref[...]
                for g in range(q_per_kv):
                    s = lax.dot_general(q_s[g], k, (((1,), (1,)), ((), ())), preferred_element_type=jnp.float32) * scale
                    s = jnp.where(allowed, s, NEG_BIG)
                    m_old = m_s[g]
                    m_new = jnp.maximum(m_old, jnp.max(s, axis=-1, keepdims=True))
                    p = jnp.exp(s - m_new)
                    fix = jnp.exp(m_old - m_new)
                    l_s[g] = l_s[g] * fix + jnp.sum(p, axis=-1, keepdims=True)
                    m_s[g] = m_new
                    acc_s[g] = acc_s[g] * fix + jnp.dot(p.astype(jnp.bfloat16), v, preferred_element_type=jnp.float32)

    for g in range(q_per_kv):
        o_ref[:, g * HEAD:(g + 1) * HEAD] = (acc_s[g] / l_s[g]).astype(jnp.bfloat16)


def attention(q, cos, sin, qpos, ks, vs, kpos, kmin):
    rows, width = q.shape
    kv = ks[0].shape[1] // HEAD
    g = width // (kv * HEAD)
    nq = rows // Q_ROWS
    blocks, brows = len(ks), ks[0].shape[0]
    qmax = jnp.max(qpos.reshape(nq, Q_ROWS), axis=1)
    kspec = [pl.BlockSpec((brows, HEAD), lambda h, i, *_: (0, h))] * (2 * blocks)
    total = blocks * brows
    return pl.pallas_call(
        functools.partial(attn_kernel, blocks, g),
        out_shape=jax.ShapeDtypeStruct((rows, width), jnp.bfloat16),
        grid_spec=pltpu.PrefetchScalarGridSpec(
            num_scalar_prefetch=2,
            grid=(kv, nq),
            in_specs=[
                pl.BlockSpec((Q_ROWS, g * HEAD), lambda h, i, *_: (i, h)),
                pl.BlockSpec((Q_ROWS, HEAD), lambda h, i, *_: (i, 0)),
                pl.BlockSpec((Q_ROWS, HEAD), lambda h, i, *_: (i, 0)),
                pl.BlockSpec((Q_ROWS, 1), lambda h, i, *_: (i, 0)),
                pl.BlockSpec((1, total), lambda h, i, *_: (0, 0)),
                *kspec,
            ],
            out_specs=pl.BlockSpec((Q_ROWS, g * HEAD), lambda h, i, *_: (i, h)),
            scratch_shapes=[
                pltpu.VMEM((g, Q_ROWS, HEAD), jnp.bfloat16),
                pltpu.VMEM((g, Q_ROWS, 1), jnp.float32),
                pltpu.VMEM((g, Q_ROWS, 1), jnp.float32),
                pltpu.VMEM((g, Q_ROWS, HEAD), jnp.float32),
            ],
        ),
        cost_estimate=pl.CostEstimate(flops=4 * rows * width * total, bytes_accessed=rows * width * 4, transcendentals=rows * total * kv * g),
    )(kmin, qmax, q, cos, sin, qpos[:, None], kpos[None, :], *ks, *vs)


def dot(a, b):
    return jnp.dot(a, b, preferred_element_type=jnp.float32)


def q_kernel(row_ref, x_ref, w_ref, token_ref, o_ref):
    o_ref[...] = dot(x_ref[...], w_ref[...]).astype(jnp.bfloat16)


def project_q(x, w, row, rows, token, step=512):
    depth, width = w.shape
    return pl.pallas_call(
        q_kernel,
        out_shape=jax.ShapeDtypeStruct((rows, width), jnp.bfloat16),
        grid_spec=pltpu.PrefetchScalarGridSpec(
            num_scalar_prefetch=1,
            grid=(width // step,),
            in_specs=[pl.BlockSpec((rows, depth), lambda n, r: (r[0], 0)), pl.BlockSpec((depth, step), lambda n, r: (0, n)), ANY],
            out_specs=pl.BlockSpec((rows, step), lambda n, r: (0, n)),
        ),
        cost_estimate=pl.CostEstimate(flops=2 * rows * depth * width, bytes_accessed=2 * (rows + width) * depth, transcendentals=0),
    )(row, x, w, token)


def part_kernel(x_ref, w_ref, token_ref, o_ref):
    o_ref[...] = dot(x_ref[...], w_ref[...])


def project_out(x, w, c, cols, token, step=512):
    rows, depth = x.shape
    return pl.pallas_call(
        part_kernel,
        out_shape=jax.ShapeDtypeStruct((rows, cols), jnp.float32),
        grid=(cols // step,),
        in_specs=[pl.BlockSpec((rows, depth), lambda n: (0, 0)), pl.BlockSpec((depth, step), lambda n: (0, c * (cols // step) + n)), ANY],
        out_specs=pl.BlockSpec((rows, step), lambda n: (0, n)),
        cost_estimate=pl.CostEstimate(flops=2 * rows * depth * cols, bytes_accessed=2 * (rows + cols) * depth, transcendentals=0),
    )(x, w, token)


def final_kernel(row_ref, x_ref, w_ref, hid_ref, part_ref, token_ref, o_ref):
    total = dot(x_ref[...], w_ref[...]) + part_ref[...]
    o_ref[...] = (hid_ref[...].astype(jnp.float32) + total).astype(jnp.bfloat16)


def finish(x, w, hidden, row, part, c, cols, token, step=512):
    rows, depth = x.shape
    per = cols // step
    return pl.pallas_call(
        final_kernel,
        out_shape=jax.ShapeDtypeStruct((rows, cols), jnp.bfloat16),
        grid_spec=pltpu.PrefetchScalarGridSpec(
            num_scalar_prefetch=1,
            grid=(per,),
            in_specs=[
                pl.BlockSpec((rows, depth), lambda n, r: (0, 0)),
                pl.BlockSpec((depth, step), lambda n, r: (0, c * per + n)),
                pl.BlockSpec((rows, step), lambda n, r: (r[0], c * per + n)),
                pl.BlockSpec((rows, step), lambda n, r: (0, n)),
                ANY,
            ],
            out_specs=pl.BlockSpec((rows, step), lambda n, r: (0, n)),
        ),
        cost_estimate=pl.CostEstimate(flops=2 * rows * depth * cols, bytes_accessed=2 * (rows + cols) * depth, transcendentals=0),
    )(row, x, w, hidden, part, token)


def solution(mesh):
    cp, tp = mesh.shape["cp"], mesh.shape["tp"]
    swap_core = [(i, i ^ 1) for i in range(cp)]
    swap_chip = [(i, i ^ 2) for i in range(cp)]
    swap_tp = [(0, 1), (1, 0)]

    def gather(x):
        far = lax.ppermute(x, "cp", swap_chip)
        return [x, lax.ppermute(x, "cp", swap_core), far, lax.ppermute(far, "cp", swap_core)]

    def local_block(hidden, tok_pos, norm_gain, w_query, w_key, w_value, w_out):
        rows, width = hidden.shape
        half = rows // 2
        t = lax.axis_index("tp").astype(jnp.int32)
        own, send = t[None], 1 - t[None]
        cos, sin = rope_tables(tok_pos)
        poss = gather(tok_pos)
        kpos = jnp.concatenate(poss)
        kmin = jnp.min(kpos.reshape(-1, K_ROWS), axis=1)
        normed = rms_normed(hidden.astype(jnp.float32), norm_gain)
        k = rope(jnp.dot(normed, w_key, preferred_element_type=jnp.float32).astype(jnp.bfloat16), cos, sin)
        ks = gather(k)
        v = jnp.dot(normed, w_value, preferred_element_type=jnp.float32).astype(jnp.bfloat16)
        vs = gather(v)

        def context(row, token):
            cut = lambda a: lax.dynamic_slice_in_dim(a, row[0] * half, half, 0)
            q = project_q(normed, w_query, row, half, token)
            return attention(q, cut(cos), cut(sin), cut(tok_pos), ks, vs, kpos, kmin)

        chunks = width // COLS
        token = v
        ctx = context(send, token)
        token = ctx
        parts = []
        for c in range(chunks):
            token = project_out(ctx, w_out, c, COLS, token)
            parts.append(lax.ppermute(token, "tp", swap_tp))
        ctx = context(own, token)
        token = ctx
        out = jnp.zeros((rows, width), jnp.bfloat16)
        for c in range(chunks):
            token = finish(ctx, w_out, hidden, own, parts[c], c, COLS, token)
            other = lax.ppermute(token, "tp", swap_tp)
            out = lax.dynamic_update_slice(out, token, (own[0] * half, c * COLS))
            out = lax.dynamic_update_slice(out, other, (send[0] * half, c * COLS))
        kv = w_key.shape[1] // HEAD
        return out, k.reshape(rows, kv, HEAD), v.reshape(rows, kv, HEAD)

    row_spec = P(("dp", "cp"), None)
    cache_spec = P(("dp", "cp"), "tp", None)
    return jax.shard_map(local_block, mesh=mesh, in_specs=(row_spec, P(("dp", "cp")), P(None), P(None, "tp"), P(None, "tp"), P(None, "tp"), P("tp", None)), out_specs=(row_spec, cache_spec, cache_spec), check_vma=False)
```

```python
import functools

import jax
import jax.numpy as jnp
from jax import lax
from jax.experimental import pallas as pl
from jax.experimental.pallas import tpu as pltpu
from jax.sharding import PartitionSpec as P

HEAD = 128
THETA = 1000000
EPS = 1e-5
NEG_BIG = -1e30
EXP_SCALE = HEAD ** -0.5 * 1.4426950408889634
Q_ROWS = 128
K_ROWS = 256
PAIR = 4
STEP = 256
SLOTS = 8
COLS = 2048
ANY = pl.BlockSpec(memory_space=pl.ANY)
VMEM = pl.BlockSpec(memory_space=pltpu.VMEM)
MESH = pl.DeviceIdType.MESH


def dot(a, b):
    return jnp.dot(a, b, preferred_element_type=jnp.float32)


def rope_tables(tok_pos):
    inv_freq = 1.0 / (THETA ** (jnp.arange(0, HEAD, 2, dtype=jnp.float32) / HEAD))
    angles = tok_pos.astype(jnp.float32)[:, None] * inv_freq[None, :]
    cos, sin = jnp.cos(angles), jnp.sin(angles)
    return jnp.concatenate([cos, cos], axis=-1), jnp.concatenate([-sin, sin], axis=-1)


def rotate(x, cos, sin):
    return (x * cos + pltpu.roll(x, HEAD // 2, 1) * sin).astype(jnp.bfloat16)


def front_kernel(hid_ref, gain_ref, cos_ref, sin_ref, pos_ref, wk_ref, wv_ref, wq_ref,
                 q_ref, own_ref, kall_ref, vall_ref, pall_ref,
                 hid_s, x_s, w_s, k_s, v_s, hid_sem, w_sem, out_sem, send_sem, recv_sem):
    rows, width = hid_s.shape
    half = rows // 2
    mine = lax.axis_index("tp")
    me = lax.axis_index("cp")
    core = me + 1 - 2 * lax.rem(me, 2)
    far = lax.rem(me + 2, 4)
    nk = wk_ref.shape[1] // STEP
    nq = wq_ref.shape[1] // STEP
    first_q = 2 * nk
    part = rows // 4

    loads = [pltpu.make_async_copy(hid_ref.at[pl.ds(c * part, part), :], hid_s.at[pl.ds(c * part, part), :], hid_sem.at[c]) for c in range(4)]
    for c in loads:
        c.start()

    def weight(b):
        if b < first_q:
            w = wk_ref if b < nk else wv_ref
            return pltpu.make_async_copy(w.at[:, pl.ds((b % nk) * STEP, STEP)], w_s.at[b % SLOTS], w_sem.at[b % SLOTS])
        return q_weight(b - first_q)

    def q_weight(i):
        slot = lax.rem(i + first_q, SLOTS)
        return pltpu.make_async_copy(wq_ref.at[:, pl.ds(pl.multiple_of(i * STEP, STEP), STEP)], w_s.at[slot], w_sem.at[slot])

    for b in range(SLOTS):
        weight(b).start()

    barrier = pltpu.get_barrier_semaphore()
    for other in (core, far):
        pl.semaphore_signal(barrier, inc=1, device_id={"cp": other}, device_id_type=MESH)
    pl.semaphore_wait(barrier, 2)

    def send(n, src, dst, other):
        return pltpu.make_async_remote_copy(src_ref=src, dst_ref=dst, send_sem=send_sem.at[n], recv_sem=recv_sem.at[n], device_id={"cp": other}, device_id_type=MESH)

    far_p, core_p = send(0, pos_ref, pall_ref.at[2], far), send(1, pos_ref, pall_ref.at[1], core)
    far_k, core_k = send(2, k_s, kall_ref.at[2], far), send(3, k_s, kall_ref.at[1], core)
    far_v, core_v = send(4, v_s, vall_ref.at[2], far), send(5, v_s, vall_ref.at[1], core)
    relay_p = send(6, pall_ref.at[2], pall_ref.at[3], core)
    relay_k = send(7, kall_ref.at[2], kall_ref.at[3], core)
    relay_v = send(8, vall_ref.at[2], vall_ref.at[3], core)
    keep_p = pltpu.make_async_copy(pos_ref, pall_ref.at[0], out_sem.at[0])
    keep_k = pltpu.make_async_copy(k_s, kall_ref.at[0], out_sem.at[1])
    keep_v = pltpu.make_async_copy(v_s, vall_ref.at[0], out_sem.at[2])
    keep_x = pltpu.make_async_copy(x_s.at[mine], own_ref, out_sem.at[3])
    far_p.start()
    core_p.start()
    keep_p.start()

    group = 16
    for c in range(4):
        loads[c].wait()

        @pl.loop(0, part // group)
        def _(g, c=c):
            r = pl.multiple_of(g * group, group)
            x = hid_s[pl.ds(c * part + r, group), :].astype(jnp.float32)
            inv = lax.rsqrt(jnp.mean(x * x, axis=-1, keepdims=True) + EPS)
            x_s[c // 2, pl.ds((c % 2) * part + r, group), :] = (x * inv * gain_ref[...]).astype(jnp.bfloat16)

    keep_x.start()
    for b in range(first_q):
        weight(b).wait()
        out = dot(x_s[...].reshape(rows, width), w_s[b % SLOTS]).astype(jnp.bfloat16)
        for h in range(STEP // HEAD):
            piece = out[:, h * HEAD:(h + 1) * HEAD]
            cols = pl.ds((b % nk) * STEP + h * HEAD, HEAD)
            if b < nk:
                k_s[:, cols] = rotate(piece.astype(jnp.float32), cos_ref[...], sin_ref[...])
            else:
                v_s[:, cols] = piece
        if b == nk - 1:
            far_k.start()
            core_k.start()
            keep_k.start()
        weight(b + SLOTS).start()
    far_v.start()
    core_v.start()
    keep_v.start()

    @pl.loop(0, nq)
    def _(i):
        slot = lax.rem(i + first_q, SLOTS)
        q_weight(i).wait()
        q_ref[:, pl.ds(pl.multiple_of(i * STEP, STEP), STEP)] = dot(x_s[1 - mine], w_s[slot]).astype(jnp.bfloat16)

        @pl.when(i < nq - SLOTS)
        def _():
            q_weight(i + SLOTS).start()

        @pl.when(i == nq // 2)
        def _():
            far_p.wait_recv()
            relay_p.start()
            far_k.wait_recv()
            relay_k.start()

    far_v.wait_recv()
    relay_v.start()
    for copy in (keep_p, keep_k, keep_v, keep_x):
        copy.wait()
    for copy in (far_p, far_k, far_v):
        copy.wait_send()
    for copy in (core_p, core_k, core_v, relay_p, relay_k, relay_v):
        copy.wait()


def front(hidden, gain, cos, sin, pos, w_key, w_value, w_query):
    rows, width = hidden.shape
    half, kvw, qw = rows // 2, w_key.shape[1], w_query.shape[1]
    bf16 = jnp.bfloat16
    return pl.pallas_call(
        front_kernel,
        out_shape=(
            jax.ShapeDtypeStruct((half, qw), bf16),
            jax.ShapeDtypeStruct((half, width), bf16),
            jax.ShapeDtypeStruct((4, rows, kvw), bf16),
            jax.ShapeDtypeStruct((4, rows, kvw), bf16),
            jax.ShapeDtypeStruct((4, *pos.shape), jnp.int32),
        ),
        in_specs=[ANY, VMEM, VMEM, VMEM, VMEM, ANY, ANY, ANY],
        out_specs=(VMEM, ANY, ANY, ANY, ANY),
        scratch_shapes=[
            pltpu.VMEM((rows, width), bf16),
            pltpu.VMEM((2, half, width), bf16),
            pltpu.VMEM((SLOTS, width, STEP), bf16),
            pltpu.VMEM((rows, kvw), bf16),
            pltpu.VMEM((rows, kvw), bf16),
            pltpu.SemaphoreType.DMA((4,)),
            pltpu.SemaphoreType.DMA((SLOTS,)),
            pltpu.SemaphoreType.DMA((4,)),
            pltpu.SemaphoreType.DMA((9,)),
            pltpu.SemaphoreType.DMA((9,)),
        ],
        compiler_params=pltpu.CompilerParams(collective_id=0, has_side_effects=True, vmem_limit_bytes=62 * 1024 * 1024),
        cost_estimate=pl.CostEstimate(flops=2 * rows * width * (2 * kvw + qw // 2), bytes_accessed=2 * width * (rows + 2 * kvw + qw), transcendentals=0),
    )(hidden, gain, cos, sin, pos, w_key, w_value, w_query)


def attn_kernel(row_ref, q_ref, cos_ref, sin_ref, qpos_ref, kpos_ref, k_ref, v_ref, token_ref, o_ref, k_s, vt_s, kp_s, q_s, m_s, l_s, acc_s, min_s):
    blocks, rows = k_ref.shape[0], k_ref.shape[1]
    groups, wide = q_s.shape[0], q_s.shape[1]
    per = rows // K_ROWS
    pair = wide // Q_ROWS
    qpos = qpos_ref[...].reshape(1, Q_ROWS)

    @pl.when(pl.program_id(0) == 0)
    def _():
        for n in range(kpos_ref.shape[0]):
            kp_s[n * HEAD:(n + 1) * HEAD, :] = jnp.broadcast_to(kpos_ref[n:n + 1, :], (HEAD, HEAD)).T
        span = K_ROWS // HEAD
        for n in range(blocks * per):
            min_s[n] = jnp.min(kpos_ref[n * span:(n + 1) * span, :])
        min_s[blocks * per] = jnp.max(qpos)

    for b in range(blocks):
        for c in range(per):
            piece = slice(c * K_ROWS, (c + 1) * K_ROWS)
            k_s[b * per + c] = k_ref[b, piece, :]
            vt_s[b * per + c] = v_ref[b, piece, :].T
    for g in range(groups * pair):
        x = q_ref[:, g * HEAD:(g + 1) * HEAD].astype(jnp.float32)
        q_s[g // pair, (g % pair) * Q_ROWS:(g % pair + 1) * Q_ROWS, :] = rotate(x, cos_ref[...], sin_ref[...])
    m_s[...] = jnp.full_like(m_s, NEG_BIG)
    l_s[...] = jnp.zeros_like(l_s)
    acc_s[...] = jnp.zeros_like(acc_s)

    @pl.loop(0, blocks * per)
    def _(idx):
        @pl.when(min_s[idx] <= min_s[blocks * per])
        def _():
            k, vt = k_s[idx], vt_s[idx]
            allowed = kp_s[pl.ds(pl.multiple_of(idx * K_ROWS, K_ROWS), K_ROWS), :] <= qpos
            allowed = jnp.concatenate([allowed] * pair, axis=1)
            for g in range(groups):
                s = lax.dot_general(k, q_s[g], (((1,), (1,)), ((), ())), preferred_element_type=jnp.float32)
                s = jnp.where(allowed, s, NEG_BIG)
                m_old = m_s[g]
                m_new = jnp.maximum(m_old, jnp.max(s, axis=0, keepdims=True))
                p = jnp.exp2((s - m_new) * EXP_SCALE)
                fix = jnp.exp2((m_old - m_new) * EXP_SCALE)
                l_s[g] = l_s[g] * fix + jnp.sum(p, axis=0, keepdims=True)
                m_s[g] = m_new
                acc_s[g] = acc_s[g] * fix + dot(vt, p.astype(jnp.bfloat16))

    for g in range(groups * pair):
        cols = slice((g % pair) * Q_ROWS, (g % pair + 1) * Q_ROWS)
        o = acc_s[g // pair, :, cols] / l_s[g // pair, :, cols]
        o_ref[:, g * HEAD:(g + 1) * HEAD] = o.T.astype(jnp.bfloat16)


def attention(q, cos, sin, pos, k_all, v_all, kpos, row, r, token):
    blocks, brows, kvw = k_all.shape
    width = q.shape[1]
    kv = kvw // HEAD
    g = width // kvw
    per = q.shape[0] // Q_ROWS
    total = blocks * brows
    n = total // K_ROWS
    mine = lambda h, s: (s[0] * per + r, 0)
    kspec = pl.BlockSpec((blocks, brows, HEAD), lambda h, s: (0, 0, h))
    return pl.pallas_call(
        attn_kernel,
        out_shape=jax.ShapeDtypeStruct((Q_ROWS, width), jnp.bfloat16),
        grid_spec=pltpu.PrefetchScalarGridSpec(
            num_scalar_prefetch=1,
            grid=(kv,),
            in_specs=[
                pl.BlockSpec((Q_ROWS, g * HEAD), lambda h, s: (r, h)),
                pl.BlockSpec((Q_ROWS, HEAD), mine),
                pl.BlockSpec((Q_ROWS, HEAD), mine),
                pl.BlockSpec((None, 1, HEAD), lambda h, s: (s[0] * per + r, 0, 0)),
                pl.BlockSpec(kpos.shape, lambda h, s: (0, 0)),
                kspec,
                kspec,
                ANY,
            ],
            out_specs=pl.BlockSpec((Q_ROWS, g * HEAD), lambda h, s: (0, h)),
            scratch_shapes=[
                pltpu.VMEM((n, K_ROWS, HEAD), jnp.bfloat16),
                pltpu.VMEM((n, HEAD, K_ROWS), jnp.bfloat16),
                pltpu.VMEM((total, HEAD), jnp.int32),
                pltpu.VMEM((g // PAIR, PAIR * Q_ROWS, HEAD), jnp.bfloat16),
                pltpu.VMEM((g // PAIR, 1, PAIR * Q_ROWS), jnp.float32),
                pltpu.VMEM((g // PAIR, 1, PAIR * Q_ROWS), jnp.float32),
                pltpu.VMEM((g // PAIR, HEAD, PAIR * Q_ROWS), jnp.float32),
                pltpu.SMEM((n + 1,), jnp.int32),
            ],
        ),
        cost_estimate=pl.CostEstimate(flops=4 * Q_ROWS * width * total, bytes_accessed=Q_ROWS * width * 4, transcendentals=Q_ROWS * total * kv * g),
    )(row, q, cos, sin, pos[:, None, :], kpos, k_all, v_all, token)


def q_kernel(x_ref, w_ref, token_ref, o_ref):
    o_ref[...] = dot(x_ref[...], w_ref[...]).astype(jnp.bfloat16)


def project_q(x, w, token, step=512):
    rows = x.shape[0]
    depth, width = w.shape
    return pl.pallas_call(
        q_kernel,
        out_shape=jax.ShapeDtypeStruct((rows, width), jnp.bfloat16),
        grid=(width // step,),
        in_specs=[pl.BlockSpec((rows, depth), lambda n: (0, 0)), pl.BlockSpec((depth, step), lambda n: (0, n)), ANY],
        out_specs=pl.BlockSpec((rows, step), lambda n: (0, n)),
        cost_estimate=pl.CostEstimate(flops=2 * rows * depth * width, bytes_accessed=2 * (rows + width) * depth, transcendentals=0),
    )(x, w, token)


def part_kernel(x_ref, w_ref, token_ref, o_ref):
    o_ref[...] = dot(x_ref[...], w_ref[...])


def project_out(x, w, c, cols, token, step=512):
    rows, depth = x.shape
    return pl.pallas_call(
        part_kernel,
        out_shape=jax.ShapeDtypeStruct((rows, cols), jnp.float32),
        grid=(cols // step,),
        in_specs=[pl.BlockSpec((rows, depth), lambda n: (0, 0)), pl.BlockSpec((depth, step), lambda n: (0, c * (cols // step) + n)), ANY],
        out_specs=pl.BlockSpec((rows, step), lambda n: (0, n)),
        cost_estimate=pl.CostEstimate(flops=2 * rows * depth * cols, bytes_accessed=2 * (rows + cols) * depth, transcendentals=0),
    )(x, w, token)


def final_kernel(row_ref, xa_ref, xb_ref, w_ref, hid_ref, pa_ref, pb_ref, token_ref, o_ref):
    top = xa_ref.shape[0]
    for x_ref, p_ref, r in ((xa_ref, pa_ref, slice(0, top)), (xb_ref, pb_ref, slice(top, None))):
        total = dot(x_ref[...], w_ref[...]) + p_ref[...]
        o_ref[r, :] = (hid_ref[r, :].astype(jnp.float32) + total).astype(jnp.bfloat16)


def finish(xs, w, hidden, row, parts, c, cols, token, step=512):
    part, depth = xs[0].shape
    rows = 2 * part
    per = cols // step
    return pl.pallas_call(
        final_kernel,
        out_shape=jax.ShapeDtypeStruct((rows, cols), jnp.bfloat16),
        grid_spec=pltpu.PrefetchScalarGridSpec(
            num_scalar_prefetch=1,
            grid=(per,),
            in_specs=[
                pl.BlockSpec((part, depth), lambda n, r: (0, 0)),
                pl.BlockSpec((part, depth), lambda n, r: (0, 0)),
                pl.BlockSpec((depth, step), lambda n, r: (0, c * per + n)),
                pl.BlockSpec((rows, step), lambda n, r: (r[0], c * per + n)),
                pl.BlockSpec((part, step), lambda n, r: (0, n)),
                pl.BlockSpec((part, step), lambda n, r: (0, n)),
                ANY,
            ],
            out_specs=pl.BlockSpec((rows, step), lambda n, r: (0, n)),
        ),
        cost_estimate=pl.CostEstimate(flops=2 * rows * depth * cols, bytes_accessed=2 * (rows + cols) * depth, transcendentals=0),
    )(row, *xs, w, hidden, *parts, token)


def place_kernel(row_ref, out_ref, x_ref, o_ref):
    o_ref[...] = x_ref[...]


def place(out, x, row, c):
    rows, cols = x.shape
    step = min(cols, 1024)
    per = cols // step
    return pl.pallas_call(
        place_kernel,
        out_shape=jax.ShapeDtypeStruct(out.shape, out.dtype),
        grid_spec=pltpu.PrefetchScalarGridSpec(
            num_scalar_prefetch=1,
            grid=(per,),
            in_specs=[ANY, pl.BlockSpec((rows, step), lambda n, r: (0, n))],
            out_specs=pl.BlockSpec((rows, step), lambda n, r: (r[0], c * per + n)),
        ),
        input_output_aliases={1: 0},
        cost_estimate=pl.CostEstimate(flops=0, bytes_accessed=4 * rows * cols, transcendentals=0),
    )(row, out, x)


def solution(mesh):
    swap_tp = [(0, 1), (1, 0)]

    def local_block(hidden, tok_pos, norm_gain, w_query, w_key, w_value, w_out):
        rows, width = hidden.shape
        half = rows // 2
        kv = w_key.shape[1] // HEAD
        t = lax.axis_index("tp").astype(jnp.int32)
        own, send = t[None], 1 - t[None]
        cos, sin = rope_tables(tok_pos)
        pos = tok_pos.reshape(-1, HEAD)
        q, own_x, k_all, v_all, p_all = front(hidden, norm_gain[None, :], cos, sin, pos, w_key, w_value, w_query)
        kpos = p_all.reshape(-1, HEAD)
        chunks = width // COLS

        def context(q, row, r, token):
            return attention(q, cos, sin, pos, k_all, v_all, kpos, row, r, token)

        token = q
        parts = []
        for r in range(half // Q_ROWS):
            token = ctx = context(q, send, r, token)
            parts.append([])
            for c in range(chunks):
                token = project_out(ctx, w_out, c, COLS, token)
                parts[-1].append(lax.ppermute(token, "tp", swap_tp))
        token = q = project_q(own_x, w_query, token)
        ctxs = []
        for r in range(half // Q_ROWS):
            token = context(q, own, r, token)
            ctxs.append(token)
        out = None
        others = []
        for c in range(chunks):
            token = finish(ctxs, w_out, hidden, own, [p[c] for p in parts], c, COLS, token)
            others.append(lax.ppermute(token, "tp", swap_tp))
            out = place(jnp.zeros((rows, width), jnp.bfloat16) if out is None else out, token, own, c)
        for c in range(chunks):
            out = place(out, others[c], send, c)
        return out, k_all[0].reshape(rows, kv, HEAD), v_all[0].reshape(rows, kv, HEAD)

    row_spec = P(("dp", "cp"), None)
    cache_spec = P(("dp", "cp"), "tp", None)
    return jax.shard_map(local_block, mesh=mesh, in_specs=(row_spec, P(("dp", "cp")), P(None), P(None, "tp"), P(None, "tp"), P(None, "tp"), P("tp", None)), out_specs=(row_spec, cache_spec, cache_spec), check_vma=False)
```

```python
import functools

import jax
import jax.numpy as jnp
from jax import lax
from jax.experimental import pallas as pl
from jax.experimental.pallas import tpu as pltpu
from jax.sharding import PartitionSpec as P

HEAD = 128
THETA = 1000000
EPS = 1e-5
NEG_BIG = -1e30
EXP_SCALE = HEAD ** -0.5 * 1.4426950408889634
Q_ROWS = 128
PAIR = 2
STEP = 256
SLOTS = 8
PART_CUTS = (0, 512, 2048, 4096, 6144, 8192)
CUTS = (0, 512, 2048, 4096, 6144, 7680, 8192)
ANY = pl.BlockSpec(memory_space=pl.ANY)
VMEM = pl.BlockSpec(memory_space=pltpu.VMEM)
MESH = pl.DeviceIdType.MESH


def dot(a, b):
    return jnp.dot(a, b, preferred_element_type=jnp.float32)


def rope_tables(tok_pos):
    pairs = 2 * (jnp.arange(HEAD) % (HEAD // 2))
    inv_freq = 1.0 / (THETA ** (pairs.astype(jnp.float32) / HEAD))
    angles = tok_pos.astype(jnp.float32)[:, None] * inv_freq[None, :]
    sign = jnp.where(jnp.arange(HEAD) < HEAD // 2, -1.0, 1.0)
    return jnp.cos(angles), jnp.sin(angles) * sign[None, :]


def rotate(x, cos, sin):
    return (x * cos + pltpu.roll(x, HEAD // 2, 1) * sin).astype(jnp.bfloat16)


def front_kernel(hid_ref, gain_ref, cos_ref, sin_ref, pos_ref, wk_ref, wv_ref, wq_ref,
                 q_ref, own_ref, kall_ref, vall_ref, pall_ref,
                 hid_s, x_s, w_s, k_s, v_s, hid_sem, w_sem, out_sem, send_sem, recv_sem):
    rows, width = hid_s.shape
    half = rows // 2
    mine = lax.axis_index("tp")
    me = lax.axis_index("cp")
    core = me + 1 - 2 * lax.rem(me, 2)
    far = lax.rem(me + 2, 4)
    nk = wk_ref.shape[1] // STEP
    nq = wq_ref.shape[1] // STEP
    first_q = 2 * nk
    part = rows // 4

    loads = [pltpu.make_async_copy(hid_ref.at[pl.ds(c * part, part), :], hid_s.at[pl.ds(c * part, part), :], hid_sem.at[c]) for c in range(4)]
    loads[0].start()
    loads[1].start()

    def weight(b):
        if b < first_q:
            w = wk_ref if b < nk else wv_ref
            return pltpu.make_async_copy(w.at[:, pl.ds((b % nk) * STEP, STEP)], w_s.at[b % SLOTS], w_sem.at[b % SLOTS])
        return q_weight(b - first_q)

    def q_weight(i):
        slot = lax.rem(i + first_q, SLOTS)
        return pltpu.make_async_copy(wq_ref.at[:, pl.ds(pl.multiple_of(i * STEP, STEP), STEP)], w_s.at[slot], w_sem.at[slot])

    barrier = pltpu.get_barrier_semaphore()
    for other in (core, far):
        pl.semaphore_signal(barrier, inc=1, device_id={"cp": other}, device_id_type=MESH)
    pl.semaphore_wait(barrier, 2)

    def send(n, src, dst, other):
        return pltpu.make_async_remote_copy(src_ref=src, dst_ref=dst, send_sem=send_sem.at[n], recv_sem=recv_sem.at[n], device_id={"cp": other}, device_id_type=MESH)

    far_p, core_p = send(0, pos_ref, pall_ref.at[2], far), send(1, pos_ref, pall_ref.at[1], core)
    far_k, core_k = send(2, k_s, kall_ref.at[2], far), send(3, k_s, kall_ref.at[1], core)
    far_v, core_v = send(4, v_s, vall_ref.at[2], far), send(5, v_s, vall_ref.at[1], core)
    relay_p = send(6, pall_ref.at[2], pall_ref.at[3], core)
    relay_k = send(7, kall_ref.at[2], kall_ref.at[3], core)
    relay_v = send(8, vall_ref.at[2], vall_ref.at[3], core)
    keep_p = pltpu.make_async_copy(pos_ref, pall_ref.at[0], out_sem.at[0])
    keep_k = pltpu.make_async_copy(k_s, kall_ref.at[0], out_sem.at[1])
    keep_v = pltpu.make_async_copy(v_s, vall_ref.at[0], out_sem.at[2])
    keep_x = pltpu.make_async_copy(x_s.at[pl.ds(pl.multiple_of(mine * half, half), half), :], own_ref, out_sem.at[3])
    far_p.start()
    core_p.start()
    keep_p.start()

    group = 64
    for c in range(4):
        loads[c].wait()
        if c < 2:
            loads[c + 2].start()
        for b in ((), (), (0, 1), (2,))[c]:
            weight(b).start()

        @pl.loop(0, part // group)
        def _(g, c=c):
            r = pl.ds(pl.multiple_of(c * part + g * group, group), group)
            total = jnp.zeros((group, HEAD), jnp.float32)
            for j in range(width // HEAD):
                x = hid_s[r, j * HEAD:(j + 1) * HEAD].astype(jnp.float32)
                total += x * x
            inv = lax.rsqrt(jnp.sum(total, axis=-1, keepdims=True) * (1.0 / width) + EPS)
            inv = jnp.broadcast_to(inv, (group, HEAD))
            for j in range(width // HEAD):
                cols = slice(j * HEAD, (j + 1) * HEAD)
                x_s[r, cols] = (hid_s[r, cols].astype(jnp.float32) * inv * gain_ref[:, cols]).astype(jnp.bfloat16)

    keep_x.start()
    for b in range(first_q):
        weight(b).wait()
        weight(2 * b + 3).start()
        weight(2 * b + 4).start()

        @pl.loop(0, 2)
        def _(j, b=b):
            r = pl.ds(pl.multiple_of(j * half, half), half)
            out = dot(x_s[r, :], w_s[b % SLOTS]).astype(jnp.bfloat16)
            for h in range(STEP // HEAD):
                piece = out[:, h * HEAD:(h + 1) * HEAD]
                cols = pl.ds((b % nk) * STEP + h * HEAD, HEAD)
                if b < nk:
                    k_s[r, cols] = rotate(piece.astype(jnp.float32), cos_ref[r, :], sin_ref[r, :])
                else:
                    v_s[r, cols] = piece

        if b == nk - 1:
            far_k.start()
            core_k.start()
            keep_k.start()
    far_v.start()
    core_v.start()
    keep_v.start()

    @pl.loop(0, nq)
    def _(i):
        slot = lax.rem(i + first_q, SLOTS)
        q_weight(i).wait()

        @pl.when(i < nq - SLOTS + 1)
        def _():
            q_weight(i + SLOTS - 1).start()

        q_ref[:, pl.ds(pl.multiple_of(i * STEP, STEP), STEP)] = dot(x_s[pl.ds(pl.multiple_of((1 - mine) * half, half), half), :], w_s[slot]).astype(jnp.bfloat16)

        @pl.when(i == nq // 2)
        def _():
            far_p.wait_recv()
            relay_p.start()
            far_k.wait_recv()
            relay_k.start()

    far_v.wait_recv()
    relay_v.start()
    for copy in (keep_p, keep_k, keep_v, keep_x):
        copy.wait()
    for copy in (far_p, far_k, far_v):
        copy.wait_send()
    for copy in (core_p, core_k, core_v, relay_p, relay_k, relay_v):
        copy.wait()


def front(hidden, gain, cos, sin, pos, w_key, w_value, w_query):
    rows, width = hidden.shape
    half, kvw, qw = rows // 2, w_key.shape[1], w_query.shape[1]
    bf16 = jnp.bfloat16
    return pl.pallas_call(
        front_kernel,
        out_shape=(
            jax.ShapeDtypeStruct((half, qw), bf16),
            jax.ShapeDtypeStruct((half, width), bf16),
            jax.ShapeDtypeStruct((4, rows, kvw), bf16),
            jax.ShapeDtypeStruct((4, rows, kvw), bf16),
            jax.ShapeDtypeStruct((4, *pos.shape), jnp.int32),
        ),
        in_specs=[ANY, VMEM, VMEM, VMEM, VMEM, ANY, ANY, ANY],
        out_specs=(VMEM, ANY, ANY, ANY, ANY),
        scratch_shapes=[
            pltpu.VMEM((rows, width), bf16),
            pltpu.VMEM((rows, width), bf16),
            pltpu.VMEM((SLOTS, width, STEP), bf16),
            pltpu.VMEM((rows, kvw), bf16),
            pltpu.VMEM((rows, kvw), bf16),
            pltpu.SemaphoreType.DMA((4,)),
            pltpu.SemaphoreType.DMA((SLOTS,)),
            pltpu.SemaphoreType.DMA((4,)),
            pltpu.SemaphoreType.DMA((9,)),
            pltpu.SemaphoreType.DMA((9,)),
        ],
        compiler_params=pltpu.CompilerParams(collective_id=0, has_side_effects=True, vmem_limit_bytes=62 * 1024 * 1024),
        cost_estimate=pl.CostEstimate(flops=2 * rows * width * (2 * kvw + qw // 2), bytes_accessed=2 * width * (rows + 2 * kvw + qw), transcendentals=0),
    )(hidden, gain, cos, sin, pos, w_key, w_value, w_query)


def attn_kernel(row_ref, q_ref, cos_ref, sin_ref, qpos_ref, kpos_ref, k_ref, v_ref, token_ref, o_ref, vt_s, kp_s, q_s, s_s, m_s, l_s, acc_s, min_s):
    blocks, rows = k_ref.shape[0], k_ref.shape[1]
    groups, wide = q_s.shape[0], q_s.shape[1]
    pair = wide // Q_ROWS
    qpos = qpos_ref[...].reshape(1, Q_ROWS)

    @pl.when(pl.program_id(0) == 0)
    def _():
        span = rows // HEAD
        for b in range(blocks):
            for n in range(span):
                kp_s[b, n * HEAD:(n + 1) * HEAD, :] = jnp.broadcast_to(kpos_ref[b * span + n:b * span + n + 1, :], (HEAD, HEAD)).T
            min_s[b] = jnp.min(kpos_ref[b * span:(b + 1) * span, :])
        min_s[blocks] = jnp.max(qpos)

    for b in range(blocks):
        vt_s[b] = v_ref[b].T
    for g in range(groups * pair):
        x = q_ref[:, g * HEAD:(g + 1) * HEAD].astype(jnp.float32)
        q_s[g // pair, (g % pair) * Q_ROWS:(g % pair + 1) * Q_ROWS, :] = rotate(x, cos_ref[...], sin_ref[...])
    m_s[...] = jnp.full_like(m_s, NEG_BIG)
    l_s[...] = jnp.zeros_like(l_s)
    acc_s[...] = jnp.zeros_like(acc_s)

    @pl.loop(0, blocks)
    def _(b):
        @pl.when(min_s[b] <= min_s[blocks])
        def _():
            k = k_ref[b]
            allowed = jnp.concatenate([kp_s[b] <= qpos] * pair, axis=1)
            for g in range(groups):
                s = lax.dot_general(k, q_s[g], (((1,), (1,)), ((), ())), preferred_element_type=jnp.float32)
                s = jnp.where(allowed, s, NEG_BIG)
                s_s[b, g] = s
                m_s[g] = jnp.maximum(m_s[g], jnp.max(s.reshape(rows // 8, 8, wide), axis=0))

    for g in range(groups):
        m_s[g] = jnp.broadcast_to(jnp.max(m_s[g], axis=0, keepdims=True), (8, wide)) * EXP_SCALE

    @pl.loop(0, blocks)
    def _(b):
        @pl.when(min_s[b] <= min_s[blocks])
        def _():
            vt = vt_s[b]
            for g in range(groups):
                p = jnp.exp2(s_s[b, g].reshape(rows // 8, 8, wide) * EXP_SCALE - m_s[g][None])
                l_s[g] += jnp.sum(p, axis=0)
                acc_s[g] += dot(vt, p.reshape(rows, wide).astype(jnp.bfloat16))

    for g in range(groups * pair):
        cols = slice((g % pair) * Q_ROWS, (g % pair + 1) * Q_ROWS)
        o = acc_s[g // pair, :, cols] / jnp.sum(l_s[g // pair, :, cols], axis=0, keepdims=True)
        o_ref[:, g * HEAD:(g + 1) * HEAD] = o.T.astype(jnp.bfloat16)


def attention(q, cos, sin, pos, k_all, v_all, kpos, row, r, token):
    blocks, brows, kvw = k_all.shape
    width = q.shape[1]
    kv = kvw // HEAD
    g = width // kvw
    per = q.shape[0] // Q_ROWS
    total = blocks * brows
    wide = PAIR * Q_ROWS
    mine = lambda h, s: (s[0] * per + r, 0)
    kspec = pl.BlockSpec((blocks, brows, HEAD), lambda h, s: (0, 0, h))
    return pl.pallas_call(
        attn_kernel,
        out_shape=jax.ShapeDtypeStruct((Q_ROWS, width), jnp.bfloat16),
        grid_spec=pltpu.PrefetchScalarGridSpec(
            num_scalar_prefetch=1,
            grid=(kv,),
            in_specs=[
                pl.BlockSpec((Q_ROWS, g * HEAD), lambda h, s: (r, h)),
                pl.BlockSpec((Q_ROWS, HEAD), mine),
                pl.BlockSpec((Q_ROWS, HEAD), mine),
                pl.BlockSpec((None, 1, HEAD), lambda h, s: (s[0] * per + r, 0, 0)),
                pl.BlockSpec(kpos.shape, lambda h, s: (0, 0)),
                kspec,
                kspec,
                ANY,
            ],
            out_specs=pl.BlockSpec((Q_ROWS, g * HEAD), lambda h, s: (0, h)),
            scratch_shapes=[
                pltpu.VMEM((blocks, HEAD, brows), jnp.bfloat16),
                pltpu.VMEM((blocks, brows, HEAD), jnp.int32),
                pltpu.VMEM((g // PAIR, wide, HEAD), jnp.bfloat16),
                pltpu.VMEM((blocks, g // PAIR, brows, wide), jnp.float32),
                pltpu.VMEM((g // PAIR, 8, wide), jnp.float32),
                pltpu.VMEM((g // PAIR, 8, wide), jnp.float32),
                pltpu.VMEM((g // PAIR, HEAD, wide), jnp.float32),
                pltpu.SMEM((blocks + 1,), jnp.int32),
            ],
        ),
        cost_estimate=pl.CostEstimate(flops=4 * Q_ROWS * width * total, bytes_accessed=Q_ROWS * width * 4, transcendentals=Q_ROWS * total * kv * g),
    )(row, q, cos, sin, pos[:, None, :], kpos, k_all, v_all, token)


def q_kernel(x_ref, w_ref, token_ref, o_ref):
    o_ref[...] = dot(x_ref[...], w_ref[...]).astype(jnp.bfloat16)


def project_q(x, w, token, step=512):
    rows = x.shape[0]
    depth, width = w.shape
    return pl.pallas_call(
        q_kernel,
        out_shape=jax.ShapeDtypeStruct((rows, width), jnp.bfloat16),
        grid=(width // step,),
        in_specs=[pl.BlockSpec((rows, depth), lambda n: (0, 0)), pl.BlockSpec((depth, step), lambda n: (0, n)), ANY],
        out_specs=pl.BlockSpec((rows, step), lambda n: (0, n)),
        cost_estimate=pl.CostEstimate(flops=2 * rows * depth * width, bytes_accessed=2 * (rows + width) * depth, transcendentals=0),
    )(x, w, token)


def part_kernel(x_ref, w_ref, token_ref, o_ref):
    o_ref[...] = dot(x_ref[...], w_ref[...])


def project_out(x, w, start, cols, token, step=512):
    rows, depth = x.shape
    return pl.pallas_call(
        part_kernel,
        out_shape=jax.ShapeDtypeStruct((rows, cols), jnp.float32),
        grid=(cols // step,),
        in_specs=[pl.BlockSpec((rows, depth), lambda n: (0, 0)), pl.BlockSpec((depth, step), lambda n: (0, start // step + n)), ANY],
        out_specs=pl.BlockSpec((rows, step), lambda n: (0, n)),
        cost_estimate=pl.CostEstimate(flops=2 * rows * depth * cols, bytes_accessed=2 * (rows + cols) * depth, transcendentals=0),
    )(x, w, token)


def final_kernel(row_ref, xa_ref, xb_ref, w_ref, hid_ref, pa_ref, pb_ref, *rest):
    final_ref, o_ref = rest[-2:]
    top = xa_ref.shape[0]
    for x_ref, p_ref, r in ((xa_ref, pa_ref, slice(0, top)), (xb_ref, pb_ref, slice(top, None))):
        total = dot(x_ref[...], w_ref[...]) + p_ref[...]
        final = (hid_ref[r, :].astype(jnp.float32) + total).astype(jnp.bfloat16)
        final_ref[r, :] = final
        o_ref[r, :] = final


def finish(xs, w, hidden, row, parts, offset, start, cols, out, step=512):
    part, depth = xs[0].shape
    rows = 2 * part
    first, skip = start // step, offset // step
    block = pl.BlockSpec((rows, step), lambda n, r: (r[0], first + n))
    return pl.pallas_call(
        final_kernel,
        out_shape=(jax.ShapeDtypeStruct((rows, cols), jnp.bfloat16), jax.ShapeDtypeStruct(hidden.shape, jnp.bfloat16)),
        grid_spec=pltpu.PrefetchScalarGridSpec(
            num_scalar_prefetch=1,
            grid=(cols // step,),
            in_specs=[
                pl.BlockSpec((part, depth), lambda n, r: (0, 0)),
                pl.BlockSpec((part, depth), lambda n, r: (0, 0)),
                pl.BlockSpec((depth, step), lambda n, r: (0, first + n)),
                block,
                pl.BlockSpec((part, step), lambda n, r: (0, skip + n)),
                pl.BlockSpec((part, step), lambda n, r: (0, skip + n)),
                *([] if out is None else [ANY]),
            ],
            out_specs=(pl.BlockSpec((rows, step), lambda n, r: (0, n)), block),
        ),
        input_output_aliases={} if out is None else {7: 1},
        cost_estimate=pl.CostEstimate(flops=2 * rows * depth * cols, bytes_accessed=2 * (rows + cols) * depth, transcendentals=0),
    )(row, *xs, w, hidden, *parts, *([] if out is None else [out]))


def place_kernel(cuts, row_ref, *refs):
    xs, o_ref = refs[:len(cuts) - 1], refs[-1]
    for x_ref, start, end in zip(xs, cuts, cuts[1:]):
        o_ref[:, start:end] = x_ref[...]


def place(out, pieces, row):
    rows = pieces[0].shape[0]
    step = 64
    per = rows // step
    return pl.pallas_call(
        functools.partial(place_kernel, CUTS),
        out_shape=jax.ShapeDtypeStruct(out.shape, out.dtype),
        grid_spec=pltpu.PrefetchScalarGridSpec(
            num_scalar_prefetch=1,
            grid=(per,),
            in_specs=[*(pl.BlockSpec((step, x.shape[1]), lambda n, r: (n, 0)) for x in pieces), ANY],
            out_specs=pl.BlockSpec((step, out.shape[1]), lambda n, r: (r[0] * per + n, 0)),
        ),
        input_output_aliases={1 + len(pieces): 0},
        cost_estimate=pl.CostEstimate(flops=0, bytes_accessed=4 * rows * out.shape[1], transcendentals=0),
    )(row, *pieces, out)


def solution(mesh):
    swap_tp = [(0, 1), (1, 0)]

    def local_block(hidden, tok_pos, norm_gain, w_query, w_key, w_value, w_out):
        rows, width = hidden.shape
        half = rows // 2
        kv = w_key.shape[1] // HEAD
        t = lax.axis_index("tp").astype(jnp.int32)
        own, send = t[None], 1 - t[None]
        cos, sin = rope_tables(tok_pos)
        pos = tok_pos.reshape(-1, HEAD)
        q, own_x, k_all, v_all, p_all = front(hidden, norm_gain[None, :], cos, sin, pos, w_key, w_value, w_query)
        kpos = p_all.reshape(-1, HEAD)
        chunks = [(a, b - a) for a, b in zip(CUTS, CUTS[1:])]
        part_chunks = [(a, b - a) for a, b in zip(PART_CUTS, PART_CUTS[1:])]
        home = [max(i for i, a in enumerate(PART_CUTS[:-1]) if a <= start) for start, _ in chunks]

        def context(q, row, r, token):
            return attention(q, cos, sin, pos, k_all, v_all, kpos, row, r, token)

        token = q
        parts = []
        for r in range(half // Q_ROWS):
            token = ctx = context(q, send, r, token)
            parts.append([])
            for start, cols in part_chunks:
                token = project_out(ctx, w_out, start, cols, token)
                parts[-1].append(lax.ppermute(token, "tp", swap_tp))
        token = q = project_q(own_x, w_query, token)
        ctxs = []
        for r in range(half // Q_ROWS):
            token = context(q, own, r, token)
            ctxs.append(token)
        out = None
        others = []
        for (start, cols), c in zip(chunks, home):
            final, out = finish(ctxs, w_out, hidden, own, [p[c] for p in parts], start - PART_CUTS[c], start, cols, out)
            others.append(lax.ppermute(final, "tp", swap_tp))
        out = place(out, others, send)
        return out, k_all[0].reshape(rows, kv, HEAD), v_all[0].reshape(rows, kv, HEAD)

    row_spec = P(("dp", "cp"), None)
    cache_spec = P(("dp", "cp"), "tp", None)
    return jax.shard_map(local_block, mesh=mesh, in_specs=(row_spec, P(("dp", "cp")), P(None), P(None, "tp"), P(None, "tp"), P(None, "tp"), P("tp", None)), out_specs=(row_spec, cache_spec, cache_spec), check_vma=False)
```

```python
import functools

import jax
import jax.numpy as jnp
from jax import lax
from jax.experimental import pallas as pl
from jax.experimental.pallas import tpu as pltpu
from jax.sharding import PartitionSpec as P


HEAD = 128
THETA = 1000000
EPS = 1e-5
NEG_BIG = -1e30
EXP_SCALE = HEAD ** -0.5 * 1.4426950408889634
Q_ROWS = 128
PAIR = 2
STEP = 256
SLOTS = 8
CUTS = (0, 1024, 3072, 5120, 7168, 8192)
ANY = pl.BlockSpec(memory_space=pl.ANY)
VMEM = pl.BlockSpec(memory_space=pltpu.VMEM)
MESH = pl.DeviceIdType.MESH


def dot(a, b):
    return jnp.dot(a, b, preferred_element_type=jnp.float32)


def rope_rows():
    half = HEAD // 2
    inv_freq = 1.0 / (THETA ** ((2 * (jnp.arange(HEAD) % half)).astype(jnp.float32) / HEAD))
    return jnp.stack([inv_freq, jnp.where(jnp.arange(HEAD) < half, -1.0, 1.0)])


def rotate(x, cos, sin):
    return (x * cos + pltpu.roll(x, HEAD // 2, 1) * sin).astype(jnp.bfloat16)


def front_kernel(hid_ref, gain_ref, rope_ref, pos_ref, wk_ref, wv_ref, wq_ref,
                 q_ref, cos_ref, sin_ref, v_ref, own_ref, kall_ref, vall_ref, pall_ref,
                 hid_s, x_s, w_s, k_s, vt_s, hid_sem, w_sem, out_sem, send_sem, recv_sem):
    rows, width = hid_s.shape
    half = rows // 2
    mine = lax.axis_index("tp")
    me = lax.axis_index("cp")
    core = me + 1 - 2 * lax.rem(me, 2)
    far = lax.rem(me + 2, 4)
    nk = wk_ref.shape[1] // STEP
    nq = wq_ref.shape[1] // STEP
    first_q = 2 * nk
    part = rows // 4

    loads = [pltpu.make_async_copy(hid_ref.at[pl.ds(c * part, part), :], hid_s.at[pl.ds(c * part, part), :], hid_sem.at[c]) for c in range(4)]
    loads[0].start()
    loads[1].start()

    def weight(b):
        if b < first_q:
            w = wk_ref if b < nk else wv_ref
            return pltpu.make_async_copy(w.at[:, pl.ds((b % nk) * STEP, STEP)], w_s.at[b % SLOTS], w_sem.at[b % SLOTS])
        return q_weight(b - first_q)

    def q_weight(i):
        slot = lax.rem(i + first_q, SLOTS)
        return pltpu.make_async_copy(wq_ref.at[:, pl.ds(pl.multiple_of(i * STEP, STEP), STEP)], w_s.at[slot], w_sem.at[slot])

    barrier = pltpu.get_barrier_semaphore()
    for other in (core, far):
        pl.semaphore_signal(barrier, inc=1, device_id={"cp": other}, device_id_type=MESH)
    pl.semaphore_wait(barrier, 2)

    def send(n, src, dst, other):
        return pltpu.make_async_remote_copy(src_ref=src, dst_ref=dst, send_sem=send_sem.at[n], recv_sem=recv_sem.at[n], device_id={"cp": other}, device_id_type=MESH)

    far_p, core_p = send(0, pos_ref, pall_ref.at[2], far), send(1, pos_ref, pall_ref.at[1], core)
    relay_p = send(2, pall_ref.at[2], pall_ref.at[3], core)
    to_far, to_core, relay = [], [], []
    for b in range(first_q):
        cut = pl.ds((b % nk) * STEP, STEP)
        at = (slice(None), cut) if b < nk else (cut, slice(None))
        src, dst = (k_s, kall_ref) if b < nk else (vt_s, vall_ref)
        to_far.append(send(3 + 3 * b, src.at[at], dst.at[(2, *at)], far))
        to_core.append(send(4 + 3 * b, src.at[at], dst.at[(1, *at)], core))
        relay.append(send(5 + 3 * b, dst.at[(2, *at)], dst.at[(3, *at)], core))
    keep_p = pltpu.make_async_copy(pos_ref, pall_ref.at[0], out_sem.at[0])
    keep_k = pltpu.make_async_copy(k_s, kall_ref.at[0], out_sem.at[1])
    keep_v = pltpu.make_async_copy(vt_s, vall_ref.at[0], out_sem.at[2])
    keep_x = pltpu.make_async_copy(x_s.at[pl.ds(pl.multiple_of(mine * half, half), half), :], own_ref, out_sem.at[3])
    far_p.start()
    core_p.start()
    keep_p.start()
    for c in range(4):
        angle = jnp.broadcast_to(pos_ref[c:c + 1, :], (HEAD, HEAD)).T.astype(jnp.float32) * rope_ref[0:1, :]
        cos_ref[c * HEAD:(c + 1) * HEAD, :] = jnp.cos(angle)
        sin_ref[c * HEAD:(c + 1) * HEAD, :] = jnp.sin(angle) * rope_ref[1:2, :]

    group = 64
    for c in range(4):
        loads[c].wait()
        if c < 2:
            loads[c + 2].start()
        for b in ((), (), (0, 1), (2,))[c]:
            weight(b).start()

        @pl.loop(0, part // group)
        def _(g, c=c):
            r = pl.ds(pl.multiple_of(c * part + g * group, group), group)
            total = jnp.zeros((group, HEAD), jnp.float32)
            for j in range(width // HEAD):
                x = hid_s[r, j * HEAD:(j + 1) * HEAD].astype(jnp.float32)
                total += x * x
            inv = lax.rsqrt(jnp.sum(total, axis=-1, keepdims=True) * (1.0 / width) + EPS)
            inv = jnp.broadcast_to(inv, (group, HEAD))
            for j in range(width // HEAD):
                cols = slice(j * HEAD, (j + 1) * HEAD)
                x_s[r, cols] = (hid_s[r, cols].astype(jnp.float32) * inv * gain_ref[:, cols]).astype(jnp.bfloat16)

    for b in range(first_q):
        weight(b).wait()
        weight(2 * b + 3).start()
        weight(2 * b + 4).start()

        @pl.loop(0, 2)
        def _(j, b=b):
            r = pl.ds(pl.multiple_of(j * half, half), half)
            out = dot(x_s[r, :], w_s[b % SLOTS]).astype(jnp.bfloat16)
            for h in range(STEP // HEAD):
                piece = out[:, h * HEAD:(h + 1) * HEAD]
                cols = pl.ds((b % nk) * STEP + h * HEAD, HEAD)
                if b < nk:
                    k_s[r, cols] = rotate(piece.astype(jnp.float32), cos_ref[r, :], sin_ref[r, :])
                else:
                    v_ref[r, cols] = piece
                    vt_s[cols, r] = piece.T

        to_far[b].start()
        to_core[b].start()
        if b == nk - 1:
            keep_k.start()
    keep_v.start()

    @pl.loop(0, nq)
    def _(i):
        slot = lax.rem(i + first_q, SLOTS)
        q_weight(i).wait()

        @pl.when(i < nq - SLOTS + 1)
        def _():
            q_weight(i + SLOTS - 1).start()

        r = pl.ds(pl.multiple_of((1 - mine) * half, half), half)
        q_ref[:, pl.ds(pl.multiple_of(i * STEP, STEP), STEP)] = dot(x_s[r, :], w_s[slot]).astype(jnp.bfloat16)

        @pl.when(i == 1)
        def _():
            keep_x.start()

        for b, turn in enumerate((3, 6, 10, 14)):
            @pl.when(i == turn)
            def _(b=b):
                if b == 0:
                    far_p.wait_recv()
                    relay_p.start()
                to_far[b].wait_recv()
                relay[b].start()

    for copy in (keep_p, keep_k, keep_v, keep_x):
        copy.wait()
    for copy in (far_p, *to_far):
        copy.wait_send()
    for copy in (core_p, relay_p, *to_core, *relay):
        copy.wait()


def front(hidden, gain, rope, pos, w_key, w_value, w_query):
    rows, width = hidden.shape
    half, kvw, qw = rows // 2, w_key.shape[1], w_query.shape[1]
    bf16 = jnp.bfloat16
    return pl.pallas_call(
        front_kernel,
        out_shape=(
            jax.ShapeDtypeStruct((half, qw), bf16),
            jax.ShapeDtypeStruct((rows, HEAD), jnp.float32),
            jax.ShapeDtypeStruct((rows, HEAD), jnp.float32),
            jax.ShapeDtypeStruct((rows, kvw), bf16),
            jax.ShapeDtypeStruct((half, width), bf16),
            jax.ShapeDtypeStruct((4, rows, kvw), bf16),
            jax.ShapeDtypeStruct((4, kvw, rows), bf16),
            jax.ShapeDtypeStruct((4, *pos.shape), jnp.int32),
        ),
        in_specs=[ANY, VMEM, VMEM, VMEM, ANY, ANY, ANY],
        out_specs=(VMEM, VMEM, VMEM, VMEM, ANY, ANY, ANY, ANY),
        scratch_shapes=[
            pltpu.VMEM((rows, width), bf16),
            pltpu.VMEM((rows, width), bf16),
            pltpu.VMEM((SLOTS, width, STEP), bf16),
            pltpu.VMEM((rows, kvw), bf16),
            pltpu.VMEM((kvw, rows), bf16),
            pltpu.SemaphoreType.DMA((4,)),
            pltpu.SemaphoreType.DMA((SLOTS,)),
            pltpu.SemaphoreType.DMA((4,)),
            pltpu.SemaphoreType.DMA((3 + 6 * kvw // STEP,)),
            pltpu.SemaphoreType.DMA((3 + 6 * kvw // STEP,)),
        ],
        compiler_params=pltpu.CompilerParams(collective_id=0, has_side_effects=True, vmem_limit_bytes=62 * 1024 * 1024),
        cost_estimate=pl.CostEstimate(flops=2 * rows * width * (2 * kvw + qw // 2), bytes_accessed=2 * width * (rows + 2 * kvw + qw), transcendentals=0),
    )(hidden, gain, rope, pos, w_key, w_value, w_query)


def attn_kernel(lead, row_ref, q_ref, cos_ref, sin_ref, qpos_ref, kpos_ref, k_ref, vt_ref, token_ref, *rest):
    if lead:
        w_ref, o_ref, part_ref, kp_s, q_s, s_s, m_s, l_s, acc_s, min_s, w_s, ctx_s, w_sem = rest
        load = pltpu.make_async_copy(w_ref.at[:, 0:lead], w_s, w_sem)
    else:
        o_ref, kp_s, q_s, s_s, m_s, l_s, acc_s, min_s = rest
    blocks, rows = k_ref.shape[0], k_ref.shape[1]
    groups, wide = acc_s.shape[0], acc_s.shape[2]
    pair = wide // Q_ROWS
    qpos = qpos_ref[...].reshape(1, Q_ROWS)

    @pl.when(pl.program_id(0) == 0)
    def _():
        if lead:
            load.start()
        span = rows // HEAD
        for b in range(blocks):
            for n in range(span):
                kp_s[b, n * HEAD:(n + 1) * HEAD, :] = jnp.broadcast_to(kpos_ref[b * span + n:b * span + n + 1, :], (HEAD, HEAD)).T
            min_s[b] = jnp.min(kpos_ref[b * span:(b + 1) * span, :])

    min_s[blocks] = jnp.max(qpos)
    for g in range(groups * pair):
        x = q_ref[:, g * HEAD:(g + 1) * HEAD].astype(jnp.float32)
        q_s[g // pair, (g % pair) * Q_ROWS:(g % pair + 1) * Q_ROWS, :] = rotate(x, cos_ref[...], sin_ref[...])
    m_s[...] = jnp.full_like(m_s, NEG_BIG)
    l_s[...] = jnp.zeros_like(l_s)
    acc_s[...] = jnp.zeros_like(acc_s)

    @pl.loop(0, blocks)
    def _(b):
        @pl.when(min_s[b] <= min_s[blocks])
        def _():
            k = k_ref[b]
            allowed = jnp.concatenate([kp_s[b] <= qpos] * pair, axis=1)
            for g in range(groups):
                s = lax.dot_general(k, q_s[g], (((1,), (1,)), ((), ())), preferred_element_type=jnp.float32)
                s = jnp.where(allowed, s, NEG_BIG)
                s_s[b, g] = s
                m_s[g] = jnp.maximum(m_s[g], jnp.max(s.reshape(rows // 8, 8, wide), axis=0))

    for g in range(groups):
        m_s[g] = jnp.broadcast_to(jnp.max(m_s[g], axis=0, keepdims=True), (8, wide)) * EXP_SCALE

    @pl.loop(0, blocks)
    def _(b):
        @pl.when(min_s[b] <= min_s[blocks])
        def _():
            vt = vt_ref[b]
            for g in range(groups):
                p = jnp.exp2(s_s[b, g].reshape(rows // 8, 8, wide) * EXP_SCALE - m_s[g][None])
                l_s[g] += jnp.sum(p, axis=0)
                acc_s[g] += dot(vt, p.reshape(rows, wide).astype(jnp.bfloat16))

    for g in range(groups * pair):
        cols = slice((g % pair) * Q_ROWS, (g % pair + 1) * Q_ROWS)
        o = acc_s[g // pair, :, cols] / jnp.sum(l_s[g // pair, :, cols], axis=0, keepdims=True)
        o_ref[:, g * HEAD:(g + 1) * HEAD] = o.T.astype(jnp.bfloat16)

    if lead:
        ctx_s[pl.program_id(0)] = o_ref[...]

        @pl.when(pl.program_id(0) == pl.num_programs(0) - 1)
        def _():
            load.wait()
            ctx = jnp.concatenate([ctx_s[n] for n in range(ctx_s.shape[0])], axis=1)
            part_ref[...] = dot(ctx, w_s[...])


def attention(q, r, count, cos, sin, pos, k_all, vt_all, kpos, block, token, w_out=None, lead=0):
    blocks, brows, kvw = k_all.shape
    width = q.shape[1]
    rows = count * Q_ROWS
    per = q.shape[0] // Q_ROWS
    kv = kvw // HEAD
    g = width // kvw
    wide = PAIR * Q_ROWS
    table = pl.BlockSpec((Q_ROWS, HEAD), lambda n, s: (s[0] * per + r + lax.div(n, kv), 0))
    unit = lambda first: pl.BlockSpec((Q_ROWS, g * HEAD), lambda n, s: (first + lax.div(n, kv), lax.rem(n, kv)))
    return pl.pallas_call(
        functools.partial(attn_kernel, lead),
        out_shape=(jax.ShapeDtypeStruct((rows, width), jnp.bfloat16), *([jax.ShapeDtypeStruct((rows, lead), jnp.float32)] if lead else [])),
        grid_spec=pltpu.PrefetchScalarGridSpec(
            num_scalar_prefetch=1,
            grid=(count * kv,),
            in_specs=[
                unit(r),
                table,
                table,
                pl.BlockSpec((None, 1, HEAD), lambda n, s: (s[0] * per + r + lax.div(n, kv), 0, 0)),
                pl.BlockSpec(kpos.shape, lambda n, s: (0, 0)),
                pl.BlockSpec((blocks, brows, HEAD), lambda n, s: (0, 0, lax.rem(n, kv))),
                pl.BlockSpec((blocks, HEAD, brows), lambda n, s: (0, lax.rem(n, kv), 0)),
                ANY,
                *([ANY] if lead else []),
            ],
            out_specs=(unit(0), *([pl.BlockSpec((rows, lead), lambda n, s: (0, 0))] if lead else [])),
            scratch_shapes=[
                pltpu.VMEM((blocks, brows, HEAD), jnp.int32),
                pltpu.VMEM((g // PAIR, wide, HEAD), jnp.bfloat16),
                pltpu.VMEM((blocks, g // PAIR, brows, wide), jnp.float32),
                pltpu.VMEM((g // PAIR, 8, wide), jnp.float32),
                pltpu.VMEM((g // PAIR, 8, wide), jnp.float32),
                pltpu.VMEM((g // PAIR, HEAD, wide), jnp.float32),
                pltpu.SMEM((blocks + 1,), jnp.int32),
                *([pltpu.VMEM((width, lead), jnp.bfloat16), pltpu.VMEM((kv, Q_ROWS, g * HEAD), jnp.bfloat16), pltpu.SemaphoreType.DMA] if lead else []),
            ],
        ),
        cost_estimate=pl.CostEstimate(flops=4 * rows * width * blocks * brows, bytes_accessed=rows * width * 4, transcendentals=rows * blocks * brows * kv * g),
    )(block, q, cos, sin, pos[:, None, :], kpos, k_all, vt_all, token, *([w_out] if lead else []))


def q_kernel(x_ref, w_ref, token_ref, o_ref):
    o_ref[...] = dot(x_ref[...], w_ref[...]).astype(jnp.bfloat16)


def project_q(x, w, token, step=512):
    rows = x.shape[0]
    depth, width = w.shape
    return pl.pallas_call(
        q_kernel,
        out_shape=jax.ShapeDtypeStruct((rows, width), jnp.bfloat16),
        grid=(width // step,),
        in_specs=[pl.BlockSpec((rows, depth), lambda n: (0, 0)), pl.BlockSpec((depth, step), lambda n: (0, n)), ANY],
        out_specs=pl.BlockSpec((rows, step), lambda n: (0, n)),
        cost_estimate=pl.CostEstimate(flops=2 * rows * depth * width, bytes_accessed=2 * (rows + width) * depth, transcendentals=0),
    )(x, w, token)


def part_kernel(x_ref, w_ref, token_ref, o_ref):
    o_ref[...] = dot(x_ref[...], w_ref[...])


def project_out(x, w, start, cols, token, step=512):
    rows, depth = x.shape
    return pl.pallas_call(
        part_kernel,
        out_shape=jax.ShapeDtypeStruct((rows, cols), jnp.float32),
        grid=(cols // step,),
        in_specs=[pl.BlockSpec((rows, depth), lambda n: (0, 0)), pl.BlockSpec((depth, step), lambda n: (0, start // step + n)), ANY],
        out_specs=pl.BlockSpec((rows, step), lambda n: (0, n)),
        cost_estimate=pl.CostEstimate(flops=2 * rows * depth * cols, bytes_accessed=2 * (rows + cols) * depth, transcendentals=0),
    )(x, w, token)


def final_kernel(row_ref, x_ref, w_ref, hid_ref, pa_ref, pb_ref, *rest):
    final_ref, o_ref = rest[-2:]
    top = pa_ref.shape[0]
    mine = dot(x_ref[...], w_ref[...])
    for p_ref, r in ((pa_ref, slice(0, top)), (pb_ref, slice(top, 2 * top))):
        total = mine[r] + p_ref[...]
        final = (hid_ref[r, :].astype(jnp.float32) + total).astype(jnp.bfloat16)
        final_ref[r, :] = final
        o_ref[r, :] = final


def finish(x, w, hidden, row, parts, start, cols, out, step=512):
    rows, depth = x.shape
    part = rows // 2
    first = start // step
    block = pl.BlockSpec((rows, step), lambda n, r: (r[0], first + n))
    return pl.pallas_call(
        final_kernel,
        out_shape=(jax.ShapeDtypeStruct((rows, cols), jnp.bfloat16), jax.ShapeDtypeStruct(hidden.shape, jnp.bfloat16)),
        grid_spec=pltpu.PrefetchScalarGridSpec(
            num_scalar_prefetch=1,
            grid=(cols // step,),
            in_specs=[
                pl.BlockSpec((rows, depth), lambda n, r: (0, 0)),
                pl.BlockSpec((depth, step), lambda n, r: (0, first + n)),
                block,
                pl.BlockSpec((part, step), lambda n, r: (0, n)),
                pl.BlockSpec((part, step), lambda n, r: (0, n)),
                *([] if out is None else [ANY]),
            ],
            out_specs=(pl.BlockSpec((rows, step), lambda n, r: (0, n)), block),
        ),
        input_output_aliases={} if out is None else {6: 1},
        cost_estimate=pl.CostEstimate(flops=2 * rows * depth * cols, bytes_accessed=2 * (rows + cols) * depth, transcendentals=0),
    )(row, x, w, hidden, *parts, *([] if out is None else [out]))


def place_kernel(row_ref, *refs):
    xs, o_ref = refs[:-2], refs[-1]
    start = 0
    for x_ref in xs:
        o_ref[:, start:start + x_ref.shape[1]] = x_ref[...]
        start += x_ref.shape[1]


def place(out, pieces, row, start):
    rows = pieces[0].shape[0]
    cols = sum(x.shape[1] for x in pieces)
    step = 64 if cols > 1024 else rows
    per = rows // step
    return pl.pallas_call(
        place_kernel,
        out_shape=jax.ShapeDtypeStruct(out.shape, out.dtype),
        grid_spec=pltpu.PrefetchScalarGridSpec(
            num_scalar_prefetch=1,
            grid=(per,),
            in_specs=[*(pl.BlockSpec((step, x.shape[1]), lambda n, r: (n, 0)) for x in pieces), ANY],
            out_specs=pl.BlockSpec((step, cols), lambda n, r: (r[0] * per + n, start // cols)),
        ),
        input_output_aliases={1 + len(pieces): 0},
        cost_estimate=pl.CostEstimate(flops=0, bytes_accessed=4 * rows * cols, transcendentals=0),
    )(row, *pieces, out)


def solution(mesh):
    swap_tp = [(0, 1), (1, 0)]

    def then_send(kernel, *args):
        got = kernel(*args)
        out = got[0] if kernel is finish else got[1] if kernel is attention else got
        return got, lax.ppermute(out, "tp", swap_tp)

    def local_block(hidden, tok_pos, norm_gain, w_query, w_key, w_value, w_out):
        rows, _ = hidden.shape
        half = rows // 2
        kv = w_key.shape[1] // HEAD
        t = lax.axis_index("tp").astype(jnp.int32)
        own, send = t[None], 1 - t[None]
        pos = tok_pos.reshape(-1, HEAD)
        q, cos, sin, v, own_x, k_all, vt_all, p_all = front(hidden, norm_gain[None, :], rope_rows(), pos, w_key, w_value, w_query)
        kpos = p_all.reshape(-1, HEAD)
        chunks = [(a, b - a) for a, b in zip(CUTS, CUTS[1:])]
        token = q
        parts = []
        for r in range(half // Q_ROWS):
            (ctx, token), part = then_send(attention, q, r, 1, cos, sin, pos, k_all, vt_all, kpos, send, token, w_out, CUTS[1])
            parts.append([part])
            for start, cols in chunks[1:]:
                token, part = then_send(project_out, ctx, w_out, start, cols, token)
                parts[r].append(part)
        q = project_q(own_x, w_query, token)
        ctx = attention(q, 0, half // Q_ROWS, cos, sin, pos, k_all, vt_all, kpos, own, q)[0]
        out = None
        others = []
        for c, (start, cols) in enumerate(chunks):
            (_, out), other = then_send(finish, ctx, w_out, hidden, own, [p[c] for p in parts], start, cols, out)
            others.append(other)
        out = place(out, others[:-1], send, 0)
        out = place(out, others[-1:], send, CUTS[-2])
        return out, k_all[0].reshape(rows, kv, HEAD), v.reshape(rows, kv, HEAD)

    row_spec = P(("dp", "cp"), None)
    cache_spec = P(("dp", "cp"), "tp", None)

    return jax.shard_map(local_block, mesh=mesh, in_specs=(row_spec, P(("dp", "cp")), P(None), P(None, "tp"), P(None, "tp"), P(None, "tp"), P("tp", None)), out_specs=(row_spec, cache_spec, cache_spec), check_vma=False)
```

```python
import functools

import jax
import jax.numpy as jnp
from jax import lax
from jax.experimental import pallas as pl
from jax.experimental.pallas import tpu as pltpu
from jax.sharding import PartitionSpec as P


HEAD = 128
THETA = 1000000
EPS = 1e-5
NEG_BIG = -1e30
EXP_SCALE = HEAD ** -0.5 * 1.4426950408889634
Q_ROWS = 128
PAIR = 2
STEP = 256
SLOTS = 8
CUTS = (0, 1024, 3072, 5120, 7680, 8192)
ANY = pl.BlockSpec(memory_space=pl.ANY)
VMEM = pl.BlockSpec(memory_space=pltpu.VMEM)
MESH = pl.DeviceIdType.MESH


def dot(a, b):
    return jnp.dot(a, b, preferred_element_type=jnp.float32)


def rope_rows():
    half = HEAD // 2
    inv_freq = 1.0 / (THETA ** ((2 * (jnp.arange(HEAD) % half)).astype(jnp.float32) / HEAD))
    return jnp.stack([inv_freq, jnp.where(jnp.arange(HEAD) < half, -1.0, 1.0)])


def rotate(x, cos, sin):
    return (x * cos + pltpu.roll(x, HEAD // 2, 1) * sin).astype(jnp.bfloat16)


def front_kernel(hid_ref, gain_ref, rope_ref, pos_ref, wk_ref, wv_ref, wq_ref,
                 q_ref, cos_ref, sin_ref, v_ref, next_ref, own_ref, kall_ref, vall_ref, pall_ref,
                 hid_s, x_s, w_s, k_s, vt_s, hid_sem, w_sem, out_sem, send_sem, recv_sem):
    rows, width = hid_s.shape
    half = rows // 2
    mine = lax.axis_index("tp")
    me = lax.axis_index("cp")
    core = me + 1 - 2 * lax.rem(me, 2)
    far = lax.rem(me + 2, 4)
    nk = wk_ref.shape[1] // STEP
    nq = wq_ref.shape[1] // STEP
    first_q = 2 * nk
    part = rows // 4

    loads = [pltpu.make_async_copy(hid_ref.at[pl.ds(c * part, part), :], hid_s.at[pl.ds(c * part, part), :], hid_sem.at[c]) for c in range(4)]
    loads[0].start()
    loads[1].start()

    def weight(b):
        if b < first_q:
            w = wk_ref if b < nk else wv_ref
            return pltpu.make_async_copy(w.at[:, pl.ds((b % nk) * STEP, STEP)], w_s.at[b % SLOTS], w_sem.at[b % SLOTS])
        return q_weight(b - first_q)

    def q_weight(i):
        slot = lax.rem(i + first_q, SLOTS)
        return pltpu.make_async_copy(wq_ref.at[:, pl.ds(pl.multiple_of(i * STEP, STEP), STEP)], w_s.at[slot], w_sem.at[slot])

    barrier = pltpu.get_barrier_semaphore()
    for other in (core, far):
        pl.semaphore_signal(barrier, inc=1, device_id={"cp": other}, device_id_type=MESH)
    pl.semaphore_wait(barrier, 2)

    def send(n, src, dst, other):
        return pltpu.make_async_remote_copy(src_ref=src, dst_ref=dst, send_sem=send_sem.at[n], recv_sem=recv_sem.at[n], device_id={"cp": other}, device_id_type=MESH)

    far_p, core_p = send(0, pos_ref, pall_ref.at[2], far), send(1, pos_ref, pall_ref.at[1], core)
    relay_p = send(2, pall_ref.at[2], pall_ref.at[3], core)
    to_far, to_core, relay = [], [], []
    for b in range(first_q):
        cut = pl.ds((b % nk) * STEP, STEP)
        at = (slice(None), cut) if b < nk else (cut, slice(None))
        src, dst = (k_s, kall_ref) if b < nk else (vt_s, vall_ref)
        to_far.append(send(3 + 3 * b, src.at[at], dst.at[(2, *at)], far))
        to_core.append(send(4 + 3 * b, src.at[at], dst.at[(1, *at)], core))
        relay.append(send(5 + 3 * b, dst.at[(2, *at)], dst.at[(3, *at)], core))
    keep_p = pltpu.make_async_copy(pos_ref, pall_ref.at[0], out_sem.at[0])
    keep_k = pltpu.make_async_copy(k_s, kall_ref.at[0], out_sem.at[1])
    keep_v = pltpu.make_async_copy(vt_s, vall_ref.at[0], out_sem.at[2])
    keep_x = pltpu.make_async_copy(x_s.at[pl.ds(pl.multiple_of(mine * half, half), half), :], own_ref, out_sem.at[3])
    keep_next = pltpu.make_async_copy(x_s.at[pl.ds(pl.multiple_of((1 - mine) * half + part, part), part), :], next_ref, out_sem.at[4])
    far_p.start()
    core_p.start()
    keep_p.start()
    for c in range(4):
        angle = jnp.broadcast_to(pos_ref[c:c + 1, :], (HEAD, HEAD)).T.astype(jnp.float32) * rope_ref[0:1, :]
        cos_ref[c * HEAD:(c + 1) * HEAD, :] = jnp.cos(angle)
        sin_ref[c * HEAD:(c + 1) * HEAD, :] = jnp.sin(angle) * rope_ref[1:2, :]

    group = 64
    for c in range(4):
        loads[c].wait()
        if c < 2:
            loads[c + 2].start()
        for b in ((), (), (0, 1), (2,))[c]:
            weight(b).start()

        @pl.loop(0, part // group)
        def _(g, c=c):
            r = pl.ds(pl.multiple_of(c * part + g * group, group), group)
            total = jnp.zeros((group, HEAD), jnp.float32)
            for j in range(width // HEAD):
                x = hid_s[r, j * HEAD:(j + 1) * HEAD].astype(jnp.float32)
                total += x * x
            inv = lax.rsqrt(jnp.sum(total, axis=-1, keepdims=True) * (1.0 / width) + EPS)
            inv = jnp.broadcast_to(inv, (group, HEAD))
            for j in range(width // HEAD):
                cols = slice(j * HEAD, (j + 1) * HEAD)
                x_s[r, cols] = (hid_s[r, cols].astype(jnp.float32) * inv * gain_ref[:, cols]).astype(jnp.bfloat16)

    for b in range(first_q):
        weight(b).wait()
        weight(2 * b + 3).start()
        weight(2 * b + 4).start()

        @pl.loop(0, 2)
        def _(j, b=b):
            r = pl.ds(pl.multiple_of(j * half, half), half)
            out = dot(x_s[r, :], w_s[b % SLOTS]).astype(jnp.bfloat16)
            for h in range(STEP // HEAD):
                piece = out[:, h * HEAD:(h + 1) * HEAD]
                cols = pl.ds((b % nk) * STEP + h * HEAD, HEAD)
                if b < nk:
                    k_s[r, cols] = rotate(piece.astype(jnp.float32), cos_ref[r, :], sin_ref[r, :])
                else:
                    v_ref[r, cols] = piece
                    vt_s[cols, r] = piece.T

        to_far[b].start()
        to_core[b].start()
        if b == nk - 1:
            keep_k.start()
    keep_v.start()

    @pl.loop(0, nq)
    def _(i):
        slot = lax.rem(i + first_q, SLOTS)
        q_weight(i).wait()

        @pl.when(i < nq - SLOTS + 1)
        def _():
            q_weight(i + SLOTS - 1).start()

        r = pl.ds(pl.multiple_of((1 - mine) * half, half), part)
        q_ref[:, pl.ds(pl.multiple_of(i * STEP, STEP), STEP)] = dot(x_s[r, :], w_s[slot]).astype(jnp.bfloat16)

        @pl.when(i == 1)
        def _():
            keep_next.start()
            keep_x.start()

        for b, turn in enumerate((2, 5, 9, 13)):
            @pl.when(i == turn)
            def _(b=b):
                if b == 0:
                    far_p.wait_recv()
                    relay_p.start()
                to_far[b].wait_recv()
                relay[b].start()

    for copy in (keep_p, keep_k, keep_v, keep_x, keep_next):
        copy.wait()
    for copy in (far_p, *to_far):
        copy.wait_send()
    for copy in (core_p, relay_p, *to_core, *relay):
        copy.wait()


def front(hidden, gain, rope, pos, w_key, w_value, w_query):
    rows, width = hidden.shape
    half, part, kvw, qw = rows // 2, rows // 4, w_key.shape[1], w_query.shape[1]
    bf16 = jnp.bfloat16
    return pl.pallas_call(
        front_kernel,
        out_shape=(
            jax.ShapeDtypeStruct((part, qw), bf16),
            jax.ShapeDtypeStruct((rows, HEAD), jnp.float32),
            jax.ShapeDtypeStruct((rows, HEAD), jnp.float32),
            jax.ShapeDtypeStruct((rows, kvw), bf16),
            jax.ShapeDtypeStruct((part, width), bf16),
            jax.ShapeDtypeStruct((half, width), bf16),
            jax.ShapeDtypeStruct((4, rows, kvw), bf16),
            jax.ShapeDtypeStruct((4, kvw, rows), bf16),
            jax.ShapeDtypeStruct((4, *pos.shape), jnp.int32),
        ),
        in_specs=[ANY, VMEM, VMEM, VMEM, ANY, ANY, ANY],
        out_specs=(VMEM, VMEM, VMEM, VMEM, ANY, ANY, ANY, ANY, ANY),
        scratch_shapes=[
            pltpu.VMEM((rows, width), bf16),
            pltpu.VMEM((rows, width), bf16),
            pltpu.VMEM((SLOTS, width, STEP), bf16),
            pltpu.VMEM((rows, kvw), bf16),
            pltpu.VMEM((kvw, rows), bf16),
            pltpu.SemaphoreType.DMA((4,)),
            pltpu.SemaphoreType.DMA((SLOTS,)),
            pltpu.SemaphoreType.DMA((5,)),
            pltpu.SemaphoreType.DMA((3 + 6 * kvw // STEP,)),
            pltpu.SemaphoreType.DMA((3 + 6 * kvw // STEP,)),
        ],
        compiler_params=pltpu.CompilerParams(collective_id=0, has_side_effects=True, vmem_limit_bytes=62 * 1024 * 1024),
        cost_estimate=pl.CostEstimate(flops=2 * rows * width * (2 * kvw + qw // 2), bytes_accessed=2 * width * (rows + 2 * kvw + qw), transcendentals=0),
    )(hidden, gain, rope, pos, w_key, w_value, w_query)


def attn_kernel(lead, row_ref, q_ref, cos_ref, sin_ref, qpos_ref, kpos_ref, k_ref, vt_ref, token_ref, *rest):
    if lead:
        w_ref, o_ref, part_ref, kp_s, q_s, s_s, m_s, l_s, acc_s, w_s, ctx_s, w_sem = rest
        load = pltpu.make_async_copy(w_ref.at[:, 0:lead], w_s, w_sem)
    else:
        o_ref, kp_s, q_s, s_s, m_s, l_s, acc_s = rest
    blocks, rows = k_ref.shape[0], k_ref.shape[1]
    groups, wide = acc_s.shape[0], acc_s.shape[2]
    pair = wide // Q_ROWS
    qpos = qpos_ref[...].reshape(1, Q_ROWS)

    @pl.when(pl.program_id(0) == 0)
    def _():
        if lead:
            load.start()
        span = rows // HEAD
        for b in range(blocks):
            for n in range(span):
                kp_s[b, n * HEAD:(n + 1) * HEAD, :] = jnp.broadcast_to(kpos_ref[b * span + n:b * span + n + 1, :], (HEAD, HEAD)).T

    for g in range(groups * pair):
        x = q_ref[:, g * HEAD:(g + 1) * HEAD].astype(jnp.float32)
        q_s[g // pair, (g % pair) * Q_ROWS:(g % pair + 1) * Q_ROWS, :] = rotate(x, cos_ref[...], sin_ref[...])
    m_s[...] = jnp.full_like(m_s, NEG_BIG)
    l_s[...] = jnp.zeros_like(l_s)
    acc_s[...] = jnp.zeros_like(acc_s)

    for b in range(blocks):
        k = k_ref[b]
        allowed = jnp.concatenate([kp_s[b] <= qpos] * pair, axis=1)
        for g in range(groups):
            s = lax.dot_general(k, q_s[g], (((1,), (1,)), ((), ())), preferred_element_type=jnp.float32)
            s = jnp.where(allowed, s, NEG_BIG)
            s_s[b, g] = s
            m_s[g] = jnp.maximum(m_s[g], jnp.max(s.reshape(rows // 8, 8, wide), axis=0))

    for g in range(groups):
        m_s[g] = jnp.broadcast_to(jnp.max(m_s[g], axis=0, keepdims=True), (8, wide)) * EXP_SCALE

    for b in range(blocks):
        vt = vt_ref[b]
        for g in range(groups):
            p = jnp.exp2(s_s[b, g].reshape(rows // 8, 8, wide) * EXP_SCALE - m_s[g][None])
            l_s[g] += jnp.sum(p, axis=0)
            acc_s[g] += dot(vt, p.reshape(rows, wide).astype(jnp.bfloat16))

    for g in range(groups * pair):
        cols = slice((g % pair) * Q_ROWS, (g % pair + 1) * Q_ROWS)
        o = acc_s[g // pair, :, cols] / jnp.sum(l_s[g // pair, :, cols], axis=0, keepdims=True)
        o_ref[:, g * HEAD:(g + 1) * HEAD] = o.T.astype(jnp.bfloat16)

    if lead:
        ctx_s[pl.program_id(0)] = o_ref[...]

        @pl.when(pl.program_id(0) == pl.num_programs(0) - 1)
        def _():
            load.wait()
            ctx = jnp.concatenate([ctx_s[n] for n in range(ctx_s.shape[0])], axis=1)
            part_ref[...] = dot(ctx, w_s[...])


def attention(q, cos, sin, pos, k_all, vt_all, kpos, block, token, w_out=None, lead=0):
    blocks, brows, kvw = k_all.shape
    rows, width = q.shape
    kv = kvw // HEAD
    g = width // kvw
    wide = PAIR * Q_ROWS
    table = pl.BlockSpec((Q_ROWS, HEAD), lambda n, s: (s[0] + lax.div(n, kv), 0))
    unit = pl.BlockSpec((Q_ROWS, g * HEAD), lambda n, s: (lax.div(n, kv), lax.rem(n, kv)))
    return pl.pallas_call(
        functools.partial(attn_kernel, lead),
        out_shape=(jax.ShapeDtypeStruct((rows, width), jnp.bfloat16), *([jax.ShapeDtypeStruct((rows, lead), jnp.float32)] if lead else [])),
        grid_spec=pltpu.PrefetchScalarGridSpec(
            num_scalar_prefetch=1,
            grid=(rows // Q_ROWS * kv,),
            in_specs=[
                unit,
                table,
                table,
                pl.BlockSpec((None, 1, HEAD), lambda n, s: (s[0] + lax.div(n, kv), 0, 0)),
                pl.BlockSpec(kpos.shape, lambda n, s: (0, 0)),
                pl.BlockSpec((blocks, brows, HEAD), lambda n, s: (0, 0, lax.rem(n, kv))),
                pl.BlockSpec((blocks, HEAD, brows), lambda n, s: (0, lax.rem(n, kv), 0)),
                ANY,
                *([ANY] if lead else []),
            ],
            out_specs=(unit, *([pl.BlockSpec((rows, lead), lambda n, s: (0, 0))] if lead else [])),
            scratch_shapes=[
                pltpu.VMEM((blocks, brows, HEAD), jnp.int32),
                pltpu.VMEM((g // PAIR, wide, HEAD), jnp.bfloat16),
                pltpu.VMEM((blocks, g // PAIR, brows, wide), jnp.float32),
                pltpu.VMEM((g // PAIR, 8, wide), jnp.float32),
                pltpu.VMEM((g // PAIR, 8, wide), jnp.float32),
                pltpu.VMEM((g // PAIR, HEAD, wide), jnp.float32),
                *([pltpu.VMEM((width, lead), jnp.bfloat16), pltpu.VMEM((kv, Q_ROWS, g * HEAD), jnp.bfloat16), pltpu.SemaphoreType.DMA] if lead else []),
            ],
        ),
        cost_estimate=pl.CostEstimate(flops=4 * rows * width * blocks * brows, bytes_accessed=rows * width * 4, transcendentals=rows * blocks * brows * kv * g),
    )(block, q, cos, sin, pos[:, None, :], kpos, k_all, vt_all, token, *([w_out] if lead else []))


def q_kernel(x_ref, w_ref, token_ref, o_ref):
    o_ref[...] = dot(x_ref[...], w_ref[...]).astype(jnp.bfloat16)


def project_q(x, w, token, step=512):
    rows = x.shape[0]
    depth, width = w.shape
    return pl.pallas_call(
        q_kernel,
        out_shape=jax.ShapeDtypeStruct((rows, width), jnp.bfloat16),
        grid=(width // step,),
        in_specs=[pl.BlockSpec((rows, depth), lambda n: (0, 0)), pl.BlockSpec((depth, step), lambda n: (0, n)), ANY],
        out_specs=pl.BlockSpec((rows, step), lambda n: (0, n)),
        cost_estimate=pl.CostEstimate(flops=2 * rows * depth * width, bytes_accessed=2 * (rows + width) * depth, transcendentals=0),
    )(x, w, token)


def part_kernel(x_ref, w_ref, token_ref, o_ref):
    o_ref[...] = dot(x_ref[...], w_ref[...])


def project_out(x, w, start, cols, token, step=512):
    rows, depth = x.shape
    return pl.pallas_call(
        part_kernel,
        out_shape=jax.ShapeDtypeStruct((rows, cols), jnp.float32),
        grid=(cols // step,),
        in_specs=[pl.BlockSpec((rows, depth), lambda n: (0, 0)), pl.BlockSpec((depth, step), lambda n: (0, start // step + n)), ANY],
        out_specs=pl.BlockSpec((rows, step), lambda n: (0, n)),
        cost_estimate=pl.CostEstimate(flops=2 * rows * depth * cols, bytes_accessed=2 * (rows + cols) * depth, transcendentals=0),
    )(x, w, token)


def final_kernel(row_ref, x_ref, w_ref, hid_ref, pa_ref, pb_ref, *rest):
    final_ref, o_ref = rest[-2:]
    top = pa_ref.shape[0]
    mine = dot(x_ref[...], w_ref[...])
    for p_ref, r in ((pa_ref, slice(0, top)), (pb_ref, slice(top, 2 * top))):
        total = mine[r] + p_ref[...]
        final = (hid_ref[r, :].astype(jnp.float32) + total).astype(jnp.bfloat16)
        final_ref[r, :] = final
        o_ref[r, :] = final


def finish(x, w, hidden, row, parts, start, cols, out, step=512):
    rows, depth = x.shape
    part = rows // 2
    first = start // step
    block = pl.BlockSpec((rows, step), lambda n, r: (r[0], first + n))
    return pl.pallas_call(
        final_kernel,
        out_shape=(jax.ShapeDtypeStruct((rows, cols), jnp.bfloat16), jax.ShapeDtypeStruct(hidden.shape, jnp.bfloat16)),
        grid_spec=pltpu.PrefetchScalarGridSpec(
            num_scalar_prefetch=1,
            grid=(cols // step,),
            in_specs=[
                pl.BlockSpec((rows, depth), lambda n, r: (0, 0)),
                pl.BlockSpec((depth, step), lambda n, r: (0, first + n)),
                block,
                pl.BlockSpec((part, step), lambda n, r: (0, n)),
                pl.BlockSpec((part, step), lambda n, r: (0, n)),
                *([] if out is None else [ANY]),
            ],
            out_specs=(pl.BlockSpec((rows, step), lambda n, r: (0, n)), block),
        ),
        input_output_aliases={} if out is None else {6: 1},
        cost_estimate=pl.CostEstimate(flops=2 * rows * depth * cols, bytes_accessed=2 * (rows + cols) * depth, transcendentals=0),
    )(row, x, w, hidden, *parts, *([] if out is None else [out]))


def place_kernel(row_ref, *refs):
    xs, o_ref = refs[:-2], refs[-1]
    start = 0
    for x_ref in xs:
        o_ref[:, start:start + x_ref.shape[1]] = x_ref[...]
        start += x_ref.shape[1]


def place(out, pieces, row, start):
    rows = pieces[0].shape[0]
    cols = sum(x.shape[1] for x in pieces)
    step = 64 if cols > 1024 else rows
    per = rows // step
    return pl.pallas_call(
        place_kernel,
        out_shape=jax.ShapeDtypeStruct(out.shape, out.dtype),
        grid_spec=pltpu.PrefetchScalarGridSpec(
            num_scalar_prefetch=1,
            grid=(per,),
            in_specs=[*(pl.BlockSpec((step, x.shape[1]), lambda n, r: (n, 0)) for x in pieces), ANY],
            out_specs=pl.BlockSpec((step, cols), lambda n, r: (r[0] * per + n, start // cols)),
        ),
        input_output_aliases={1 + len(pieces): 0},
        cost_estimate=pl.CostEstimate(flops=0, bytes_accessed=4 * rows * cols, transcendentals=0),
    )(row, *pieces, out)


def solution(mesh):
    swap_tp = [(0, 1), (1, 0)]

    def then_send(kernel, *args):
        got = kernel(*args)
        out = got[0] if kernel is finish else got[1] if kernel is attention else got
        return got, lax.ppermute(out, "tp", swap_tp)

    def local_block(hidden, tok_pos, norm_gain, w_query, w_key, w_value, w_out):
        rows, _ = hidden.shape
        kv = w_key.shape[1] // HEAD
        t = lax.axis_index("tp").astype(jnp.int32)
        own, send = t[None], 1 - t[None]
        pos = tok_pos.reshape(-1, HEAD)
        q, cos, sin, v, next_x, own_x, k_all, vt_all, p_all = front(hidden, norm_gain[None, :], rope_rows(), pos, w_key, w_value, w_query)
        kpos = p_all.reshape(-1, HEAD)
        chunks = [(a, b - a) for a, b in zip(CUTS, CUTS[1:])]
        token = q
        parts = []
        for r in range(2):
            if r > 0:
                token = q = project_q(next_x, w_query, token)
            (ctx, token), part = then_send(attention, q, cos, sin, pos, k_all, vt_all, kpos, 2 * send + r, token, w_out, CUTS[1])
            parts.append([part])
            for start, cols in chunks[1:]:
                token, part = then_send(project_out, ctx, w_out, start, cols, token)
                parts[r].append(part)
        q = project_q(own_x, w_query, token)
        ctx = attention(q, cos, sin, pos, k_all, vt_all, kpos, 2 * own, q)[0]
        out = None
        others = []
        for c, (start, cols) in enumerate(chunks):
            (_, out), other = then_send(finish, ctx, w_out, hidden, own, [p[c] for p in parts], start, cols, out)
            others.append(other)
        out = place(out, others[:-1], send, 0)
        out = place(out, others[-1:], send, CUTS[-2])
        return out, k_all[0].reshape(rows, kv, HEAD), v.reshape(rows, kv, HEAD)

    row_spec = P(("dp", "cp"), None)
    cache_spec = P(("dp", "cp"), "tp", None)

    return jax.shard_map(local_block, mesh=mesh, in_specs=(row_spec, P(("dp", "cp")), P(None), P(None, "tp"), P(None, "tp"), P(None, "tp"), P("tp", None)), out_specs=(row_spec, cache_spec, cache_spec), check_vma=False)
```

```python
import functools
import math

import jax
import jax.numpy as jnp
from jax import lax
from jax.experimental import pallas as pl
from jax.experimental.pallas import tpu as pltpu
from jax.sharding import PartitionSpec as P


HEAD = 128
THETA = 1000000
EPS = 1e-5
NEG_BIG = -1e30
EXP_SCALE = HEAD ** -0.5 * 1.4426950408889634
Q_ROWS = 128
PAIR = 2
STEP = 256
SLOTS = 8
CUTS = (0, 1024, 3072, 5120, 7680, 8192)
ANY = pl.BlockSpec(memory_space=pl.ANY)
VMEM = pl.BlockSpec(memory_space=pltpu.VMEM)
MESH = pl.DeviceIdType.MESH


def dot(a, b):
    return jnp.dot(a, b, preferred_element_type=jnp.float32)


def rope_rows():
    half = HEAD // 2
    inv_freq = 1.0 / (THETA ** ((2 * (jnp.arange(HEAD) % half)).astype(jnp.float32) / HEAD))
    return jnp.stack([inv_freq, jnp.where(jnp.arange(HEAD) < half, -1.0, 1.0)])


def rotate(x, cos, sin):
    return (x * cos + pltpu.roll(x, HEAD // 2, 1) * sin).astype(jnp.bfloat16)


def front_kernel(hid_ref, gain_ref, rope_ref, pos_ref, wk_ref, wv_ref, wq_ref,
                 q_ref, cos_ref, sin_ref, v_ref, next_ref, own_ref, kall_ref, vall_ref, pall_ref,
                 hid_s, x_s, w_s, k_s, vt_s, hid_sem, w_sem, out_sem, send_sem, recv_sem):
    rows, width = hid_s.shape
    half = rows // 2
    mine = lax.axis_index("tp")
    me = lax.axis_index("cp")
    core = me + 1 - 2 * lax.rem(me, 2)
    far = lax.rem(me + 2, 4)
    nk = wk_ref.shape[1] // STEP
    nq = wq_ref.shape[1] // STEP
    first_q = 2 * nk
    part = rows // 4

    loads = [pltpu.make_async_copy(hid_ref.at[pl.ds(c * part, part), :], hid_s.at[pl.ds(c * part, part), :], hid_sem.at[c]) for c in range(4)]
    loads[0].start()
    loads[1].start()

    def weight(b):
        if b < first_q:
            w = wk_ref if b < nk else wv_ref
            return pltpu.make_async_copy(w.at[:, pl.ds((b % nk) * STEP, STEP)], w_s.at[b % SLOTS], w_sem.at[b % SLOTS])
        return q_weight(b - first_q)

    def q_weight(i):
        slot = lax.rem(i + first_q, SLOTS)
        return pltpu.make_async_copy(wq_ref.at[:, pl.ds(pl.multiple_of(i * STEP, STEP), STEP)], w_s.at[slot], w_sem.at[slot])

    barrier = pltpu.get_barrier_semaphore()
    for other in (core, far):
        pl.semaphore_signal(barrier, inc=1, device_id={"cp": other}, device_id_type=MESH)
    pl.semaphore_wait(barrier, 2)

    def send(n, src, dst, other):
        return pltpu.make_async_remote_copy(src_ref=src, dst_ref=dst, send_sem=send_sem.at[n], recv_sem=recv_sem.at[n], device_id={"cp": other}, device_id_type=MESH)

    far_p, core_p = send(0, pos_ref, pall_ref.at[2], far), send(1, pos_ref, pall_ref.at[1], core)
    relay_p = send(2, pall_ref.at[2], pall_ref.at[3], core)
    to_far, to_core, relay = [], [], []
    pieces = [(0, pl.ds(0, half)), (0, pl.ds(half, half)), *((b, pl.ds(0, rows)) for b in range(1, first_q))]
    for n, (b, r) in enumerate(pieces):
        cut = pl.ds((b % nk) * STEP, STEP)
        at = (r, cut) if b < nk else (cut, r)
        src, dst = (k_s, kall_ref) if b < nk else (vt_s, vall_ref)
        to_far.append(send(3 + 3 * n, src.at[at], dst.at[(2, *at)], far))
        to_core.append(send(4 + 3 * n, src.at[at], dst.at[(1, *at)], core))
        relay.append(send(5 + 3 * n, dst.at[(2, *at)], dst.at[(3, *at)], core))

    def pass_on(n):
        to_far[n].start()
        to_core[n].start()

    def project(b, j):
        r = pl.ds(pl.multiple_of(j * half, half), half)
        out = dot(x_s[r, :], w_s[b % SLOTS]).astype(jnp.bfloat16)
        for h in range(STEP // HEAD):
            piece = out[:, h * HEAD:(h + 1) * HEAD]
            cols = pl.ds((b % nk) * STEP + h * HEAD, HEAD)
            if b < nk:
                k_s[r, cols] = rotate(piece.astype(jnp.float32), cos_ref[r, :], sin_ref[r, :])
            else:
                v_ref[r, cols] = piece
                vt_s[cols, r] = piece.T

    keep_p = pltpu.make_async_copy(pos_ref, pall_ref.at[0], out_sem.at[0])
    keep_k = pltpu.make_async_copy(k_s, kall_ref.at[0], out_sem.at[1])
    keep_v = pltpu.make_async_copy(vt_s, vall_ref.at[0], out_sem.at[2])
    keep_x = pltpu.make_async_copy(x_s.at[pl.ds(pl.multiple_of(mine * half, half), half), :], own_ref, out_sem.at[3])
    keep_next = pltpu.make_async_copy(x_s.at[pl.ds(pl.multiple_of((1 - mine) * half + part, part), part), :], next_ref, out_sem.at[4])
    far_p.start()
    core_p.start()
    keep_p.start()
    for c in range(4):
        angle = jnp.broadcast_to(pos_ref[c:c + 1, :], (HEAD, HEAD)).T.astype(jnp.float32) * rope_ref[0:1, :]
        cos_ref[c * HEAD:(c + 1) * HEAD, :] = jnp.cos(angle)
        sin_ref[c * HEAD:(c + 1) * HEAD, :] = jnp.sin(angle) * rope_ref[1:2, :]

    group = 64
    for c in range(4):
        loads[c].wait()
        (loads[2] if c == 1 else weight((0, 0, 1, 3)[c])).start()
        if c == 2:
            weight(2).start()
        if c == 3:
            weight(4).start()

        @pl.loop(0, part // group)
        def _(g, c=c):
            r = pl.ds(pl.multiple_of(c * part + g * group, group), group)
            total = jnp.zeros((group, HEAD), jnp.float32)
            for j in range(width // HEAD):
                x = hid_s[r, j * HEAD:(j + 1) * HEAD].astype(jnp.float32)
                total += x * x
            inv = lax.rsqrt(jnp.sum(total, axis=-1, keepdims=True) * (1.0 / width) + EPS)
            inv = jnp.broadcast_to(inv, (group, HEAD))
            for j in range(width // HEAD):
                cols = slice(j * HEAD, (j + 1) * HEAD)
                x_s[r, cols] = (hid_s[r, cols].astype(jnp.float32) * inv * gain_ref[:, cols]).astype(jnp.bfloat16)

        if c == 1:
            weight(0).wait()
            loads[3].start()
            project(0, 0)
            pass_on(0)

    weight(5).start()
    weight(6).start()
    weight(7).start()
    project(0, 1)
    pass_on(1)
    for b in range(1, first_q):
        weight(b).wait()
        weight(b + SLOTS - 1).start()

        @pl.loop(0, 2)
        def _(j, b=b):
            project(b, j)

        pass_on(b + 1)
        if b == nk - 1:
            keep_k.start()
    keep_v.start()

    @pl.loop(0, nq)
    def _(i):
        slot = lax.rem(i + first_q, SLOTS)
        q_weight(i).wait()

        @pl.when(i < nq - SLOTS + 1)
        def _():
            q_weight(i + SLOTS - 1).start()

        r = pl.ds(pl.multiple_of((1 - mine) * half, half), part)
        q_ref[:, pl.ds(pl.multiple_of(i * STEP, STEP), STEP)] = dot(x_s[r, :], w_s[slot]).astype(jnp.bfloat16)

        @pl.when(i == 1)
        def _():
            keep_next.start()
            keep_x.start()

        for turn, ready in ((1, (0, 1)), (4, (2,)), (8, (3,)), (13, (4,))):
            @pl.when(i == turn)
            def _(ready=ready):
                if 0 in ready:
                    far_p.wait_recv()
                    relay_p.start()
                for n in ready:
                    to_far[n].wait_recv()
                    relay[n].start()

    for copy in (keep_p, keep_k, keep_v, keep_x, keep_next):
        copy.wait()
    for copy in (far_p, *to_far):
        copy.wait_send()
    for copy in (core_p, relay_p, *to_core, *relay):
        copy.wait()


def front(hidden, gain, rope, pos, w_key, w_value, w_query):
    rows, width = hidden.shape
    half, part, kvw, qw = rows // 2, rows // 4, w_key.shape[1], w_query.shape[1]
    bf16 = jnp.bfloat16
    return pl.pallas_call(
        front_kernel,
        out_shape=(
            jax.ShapeDtypeStruct((part, qw), bf16),
            jax.ShapeDtypeStruct((rows, HEAD), jnp.float32),
            jax.ShapeDtypeStruct((rows, HEAD), jnp.float32),
            jax.ShapeDtypeStruct((rows, kvw), bf16),
            jax.ShapeDtypeStruct((part, width), bf16),
            jax.ShapeDtypeStruct((half, width), bf16),
            jax.ShapeDtypeStruct((4, rows, kvw), bf16),
            jax.ShapeDtypeStruct((4, kvw, rows), bf16),
            jax.ShapeDtypeStruct((4, *pos.shape), jnp.int32),
        ),
        in_specs=[ANY, VMEM, VMEM, VMEM, ANY, ANY, ANY],
        out_specs=(VMEM, VMEM, VMEM, VMEM, ANY, ANY, ANY, ANY, ANY),
        scratch_shapes=[
            pltpu.VMEM((rows, width), bf16),
            pltpu.VMEM((rows, width), bf16),
            pltpu.VMEM((SLOTS, width, STEP), bf16),
            pltpu.VMEM((rows, kvw), bf16),
            pltpu.VMEM((kvw, rows), bf16),
            pltpu.SemaphoreType.DMA((4,)),
            pltpu.SemaphoreType.DMA((SLOTS,)),
            pltpu.SemaphoreType.DMA((5,)),
            pltpu.SemaphoreType.DMA((6 + 6 * kvw // STEP,)),
            pltpu.SemaphoreType.DMA((6 + 6 * kvw // STEP,)),
        ],
        compiler_params=pltpu.CompilerParams(collective_id=0, has_side_effects=True, vmem_limit_bytes=62 * 1024 * 1024),
        cost_estimate=pl.CostEstimate(flops=2 * rows * width * (2 * kvw + qw // 2), bytes_accessed=2 * width * (rows + 2 * kvw + qw), transcendentals=0),
    )(hidden, gain, rope, pos, w_key, w_value, w_query)


def attn_kernel(lead, row_ref, q_ref, cos_ref, sin_ref, qpos_ref, kpos_ref, k_ref, vt_ref, token_ref, *rest):
    if lead:
        w_ref, o_ref, part_ref, kp_s, q_s, s_s, m_s, l_s, acc_s, w_s, ctx_s, w_sem = rest
        load = pltpu.make_async_copy(w_ref.at[:, 0:lead], w_s, w_sem)
    else:
        o_ref, kp_s, q_s, s_s, m_s, l_s, acc_s = rest
    blocks, rows = k_ref.shape[0], k_ref.shape[1]
    groups, wide = acc_s.shape[0], acc_s.shape[2]
    pair = wide // Q_ROWS
    qpos = qpos_ref[...].reshape(1, Q_ROWS)

    @pl.when(pl.program_id(0) == 0)
    def _():
        if lead:
            load.start()
        span = rows // HEAD
        for b in range(blocks):
            for n in range(span):
                kp_s[b, n * HEAD:(n + 1) * HEAD, :] = jnp.broadcast_to(kpos_ref[b * span + n:b * span + n + 1, :], (HEAD, HEAD)).T

    for g in range(groups * pair):
        x = q_ref[:, g * HEAD:(g + 1) * HEAD].astype(jnp.float32)
        q_s[g // pair, (g % pair) * Q_ROWS:(g % pair + 1) * Q_ROWS, :] = rotate(x, cos_ref[...], sin_ref[...])
    m_s[...] = jnp.full_like(m_s, NEG_BIG)
    l_s[...] = jnp.zeros_like(l_s)
    acc_s[...] = jnp.zeros_like(acc_s)

    for b in range(blocks):
        k = k_ref[b]
        allowed = jnp.concatenate([kp_s[b] <= qpos] * pair, axis=1)
        for g in range(groups):
            s = lax.dot_general(k, q_s[g], (((1,), (1,)), ((), ())), preferred_element_type=jnp.float32)
            s = jnp.where(allowed, s, NEG_BIG)
            s_s[b, g] = s
            m_s[g] = jnp.maximum(m_s[g], jnp.max(s.reshape(rows // 8, 8, wide), axis=0))

    for g in range(groups):
        m_s[g] = jnp.broadcast_to(jnp.max(m_s[g], axis=0, keepdims=True), (8, wide)) * EXP_SCALE

    for b in range(blocks):
        vt = vt_ref[b]
        for g in range(groups):
            p = jnp.exp2(s_s[b, g].reshape(rows // 8, 8, wide) * EXP_SCALE - m_s[g][None])
            l_s[g] += jnp.sum(p, axis=0)
            acc_s[g] += dot(vt, p.reshape(rows, wide).astype(jnp.bfloat16))

    for g in range(groups * pair):
        cols = slice((g % pair) * Q_ROWS, (g % pair + 1) * Q_ROWS)
        o = acc_s[g // pair, :, cols] / jnp.sum(l_s[g // pair, :, cols], axis=0, keepdims=True)
        o_ref[:, g * HEAD:(g + 1) * HEAD] = o.T.astype(jnp.bfloat16)

    if lead:
        ctx_s[pl.program_id(0)] = o_ref[...]

        @pl.when(pl.program_id(0) == pl.num_programs(0) - 1)
        def _():
            load.wait()
            ctx = jnp.concatenate([ctx_s[n] for n in range(ctx_s.shape[0])], axis=1)
            part_ref[...] = dot(ctx, w_s[...])


def attention(q, cos, sin, pos, k_all, vt_all, kpos, block, token, w_out=None, lead=0):
    blocks, brows, kvw = k_all.shape
    rows, width = q.shape
    kv = kvw // HEAD
    g = width // kvw
    wide = PAIR * Q_ROWS
    table = pl.BlockSpec((Q_ROWS, HEAD), lambda n, s: (s[0] + lax.div(n, kv), 0))
    unit = pl.BlockSpec((Q_ROWS, g * HEAD), lambda n, s: (lax.div(n, kv), lax.rem(n, kv)))
    return pl.pallas_call(
        functools.partial(attn_kernel, lead),
        out_shape=(jax.ShapeDtypeStruct((rows, width), jnp.bfloat16), *([jax.ShapeDtypeStruct((rows, lead), jnp.float32)] if lead else [])),
        grid_spec=pltpu.PrefetchScalarGridSpec(
            num_scalar_prefetch=1,
            grid=(rows // Q_ROWS * kv,),
            in_specs=[
                unit,
                table,
                table,
                pl.BlockSpec((None, 1, HEAD), lambda n, s: (s[0] + lax.div(n, kv), 0, 0)),
                pl.BlockSpec(kpos.shape, lambda n, s: (0, 0)),
                pl.BlockSpec((blocks, brows, HEAD), lambda n, s: (0, 0, lax.rem(n, kv))),
                pl.BlockSpec((blocks, HEAD, brows), lambda n, s: (0, lax.rem(n, kv), 0)),
                ANY,
                *([ANY] if lead else []),
            ],
            out_specs=(unit, *([pl.BlockSpec((rows, lead), lambda n, s: (0, 0))] if lead else [])),
            scratch_shapes=[
                pltpu.VMEM((blocks, brows, HEAD), jnp.int32),
                pltpu.VMEM((g // PAIR, wide, HEAD), jnp.bfloat16),
                pltpu.VMEM((blocks, g // PAIR, brows, wide), jnp.float32),
                pltpu.VMEM((g // PAIR, 8, wide), jnp.float32),
                pltpu.VMEM((g // PAIR, 8, wide), jnp.float32),
                pltpu.VMEM((g // PAIR, HEAD, wide), jnp.float32),
                *([pltpu.VMEM((width, lead), jnp.bfloat16), pltpu.VMEM((kv, Q_ROWS, g * HEAD), jnp.bfloat16), pltpu.SemaphoreType.DMA] if lead else []),
            ],
        ),
        cost_estimate=pl.CostEstimate(flops=4 * rows * width * blocks * brows, bytes_accessed=rows * width * 4, transcendentals=rows * blocks * brows * kv * g),
    )(block, q, cos, sin, pos[:, None, :], kpos, k_all, vt_all, token, *([w_out] if lead else []))


def q_kernel(x_ref, w_ref, token_ref, o_ref):
    o_ref[...] = dot(x_ref[...], w_ref[...]).astype(jnp.bfloat16)


def project_q(x, w, token, step=512):
    rows = x.shape[0]
    depth, width = w.shape
    return pl.pallas_call(
        q_kernel,
        out_shape=jax.ShapeDtypeStruct((rows, width), jnp.bfloat16),
        grid=(width // step,),
        in_specs=[pl.BlockSpec((rows, depth), lambda n: (0, 0)), pl.BlockSpec((depth, step), lambda n: (0, n)), ANY],
        out_specs=pl.BlockSpec((rows, step), lambda n: (0, n)),
        cost_estimate=pl.CostEstimate(flops=2 * rows * depth * width, bytes_accessed=2 * (rows + width) * depth, transcendentals=0),
    )(x, w, token)


def part_kernel(x_ref, w_ref, token_ref, o_ref):
    o_ref[...] = dot(x_ref[...], w_ref[...])


def project_out(x, w, start, cols, token, step=512):
    rows, depth = x.shape
    return pl.pallas_call(
        part_kernel,
        out_shape=jax.ShapeDtypeStruct((rows, cols), jnp.float32),
        grid=(cols // step,),
        in_specs=[pl.BlockSpec((rows, depth), lambda n: (0, 0)), pl.BlockSpec((depth, step), lambda n: (0, start // step + n)), ANY],
        out_specs=pl.BlockSpec((rows, step), lambda n: (0, n)),
        cost_estimate=pl.CostEstimate(flops=2 * rows * depth * cols, bytes_accessed=2 * (rows + cols) * depth, transcendentals=0),
    )(x, w, token)


def final_kernel(row_ref, x_ref, w_ref, hid_ref, pa_ref, pb_ref, *rest):
    final_ref, o_ref = rest[-2:]
    top = pa_ref.shape[0]
    mine = dot(x_ref[...], w_ref[...])
    for p_ref, r in ((pa_ref, slice(0, top)), (pb_ref, slice(top, 2 * top))):
        total = mine[r] + p_ref[...]
        final = (hid_ref[r, :].astype(jnp.float32) + total).astype(jnp.bfloat16)
        final_ref[r, :] = final
        o_ref[r, :] = final


def finish(x, w, hidden, row, parts, start, cols, out, step=512):
    rows, depth = x.shape
    part = rows // 2
    first = start // step
    block = pl.BlockSpec((rows, step), lambda n, r: (r[0], first + n))
    return pl.pallas_call(
        final_kernel,
        out_shape=(jax.ShapeDtypeStruct((rows, cols), jnp.bfloat16), jax.ShapeDtypeStruct(hidden.shape, jnp.bfloat16)),
        grid_spec=pltpu.PrefetchScalarGridSpec(
            num_scalar_prefetch=1,
            grid=(cols // step,),
            in_specs=[
                pl.BlockSpec((rows, depth), lambda n, r: (0, 0)),
                pl.BlockSpec((depth, step), lambda n, r: (0, first + n)),
                block,
                pl.BlockSpec((part, step), lambda n, r: (0, n)),
                pl.BlockSpec((part, step), lambda n, r: (0, n)),
                *([] if out is None else [ANY]),
            ],
            out_specs=(pl.BlockSpec((rows, step), lambda n, r: (0, n)), block),
        ),
        input_output_aliases={} if out is None else {6: 1},
        cost_estimate=pl.CostEstimate(flops=2 * rows * depth * cols, bytes_accessed=2 * (rows + cols) * depth, transcendentals=0),
    )(row, x, w, hidden, *parts, *([] if out is None else [out]))


def place_kernel(row_ref, *refs):
    xs, o_ref = refs[:-2], refs[-1]
    start = 0
    for x_ref in xs:
        o_ref[:, start:start + x_ref.shape[1]] = x_ref[...]
        start += x_ref.shape[1]


def place(out, pieces, row, start):
    rows = pieces[0].shape[0]
    cols = sum(x.shape[1] for x in pieces)
    wide = cols if start % cols == 0 else math.gcd(start, cols)
    assert wide == cols or len(pieces) == 1
    step = 64 if cols > 4096 else rows
    per = rows // step
    return pl.pallas_call(
        place_kernel,
        out_shape=jax.ShapeDtypeStruct(out.shape, out.dtype),
        grid_spec=pltpu.PrefetchScalarGridSpec(
            num_scalar_prefetch=1,
            grid=(per, cols // wide),
            in_specs=[*(pl.BlockSpec((step, x.shape[1] * wide // cols), lambda n, c, r: (n, c)) for x in pieces), ANY],
            out_specs=pl.BlockSpec((step, wide), lambda n, c, r: (r[0] * per + n, start // wide + c)),
        ),
        input_output_aliases={1 + len(pieces): 0},
        cost_estimate=pl.CostEstimate(flops=0, bytes_accessed=4 * rows * cols, transcendentals=0),
    )(row, *pieces, out)


def solution(mesh):
    swap_tp = [(0, 1), (1, 0)]

    def then_send(kernel, *args):
        got = kernel(*args)
        out = got[0] if kernel is finish else got[1] if kernel is attention else got
        return got, lax.ppermute(out, "tp", swap_tp)

    def local_block(hidden, tok_pos, norm_gain, w_query, w_key, w_value, w_out):
        rows, _ = hidden.shape
        kv = w_key.shape[1] // HEAD
        t = lax.axis_index("tp").astype(jnp.int32)
        own, send = t[None], 1 - t[None]
        pos = tok_pos.reshape(-1, HEAD)
        q, cos, sin, v, next_x, own_x, k_all, vt_all, p_all = front(hidden, norm_gain[None, :], rope_rows(), pos, w_key, w_value, w_query)
        kpos = p_all.reshape(-1, HEAD)
        chunks = [(a, b - a) for a, b in zip(CUTS, CUTS[1:])]
        token = q
        parts = []
        for r in range(2):
            if r > 0:
                token = q = project_q(next_x, w_query, token)
            (ctx, token), part = then_send(attention, q, cos, sin, pos, k_all, vt_all, kpos, 2 * send + r, token, w_out, CUTS[1])
            parts.append([part])
            for start, cols in chunks[1:]:
                token, part = then_send(project_out, ctx, w_out, start, cols, token)
                parts[r].append(part)
        q = project_q(own_x, w_query, token)
        ctx = attention(q, cos, sin, pos, k_all, vt_all, kpos, 2 * own, q)[0]
        out = None
        others = []
        for c, (start, cols) in enumerate(chunks):
            (_, out), other = then_send(finish, ctx, w_out, hidden, own, [p[c] for p in parts], start, cols, out)
            others.append(other)
        out = place(out, others[:-2], send, 0)
        out = place(out, others[-2:-1], send, CUTS[-3])
        out = place(out, others[-1:], send, CUTS[-2])
        return out, k_all[0].reshape(rows, kv, HEAD), v.reshape(rows, kv, HEAD)

    row_spec = P(("dp", "cp"), None)
    cache_spec = P(("dp", "cp"), "tp", None)

    return jax.shard_map(local_block, mesh=mesh, in_specs=(row_spec, P(("dp", "cp")), P(None), P(None, "tp"), P(None, "tp"), P(None, "tp"), P("tp", None)), out_specs=(row_spec, cache_spec, cache_spec), check_vma=False)
```
